256 devices in a mesh: seq: 32 (over y, z), head: 8 (over x, core).
Axes of the slice: x: 4, y: 4, z: 8, core: 2. Of those that a mesh axis runs over, the one named last changes fastest.
Arguments:
- tokens: bfloat16 [2, 4096, 2560], P(None, 'seq', 'head'), may hold values from -6 to 6
- token_mix: float32 [5, 2560], replicated, may hold values from 0.05 to 0.95
- receptance: bfloat16 [2560, 2560], P(None, 'head'), may hold values from -0.125 to 0.125
- key_weight: bfloat16 [2560, 2560], P(None, 'head'), may hold values from -0.125 to 0.125
- value_weight: bfloat16 [2560, 2560], P(None, 'head'), may hold values from -0.125 to 0.125
- decay_base: float32 [2560], P('head'), may hold values from -12.5 to -1.9
- decay_down_matrix: bfloat16 [2560, 96], replicated, may hold values from -0.125 to 0.125
- decay_up_matrix: bfloat16 [96, 2560], P(None, 'head'), may hold values from -0.625 to 0.625
- learn_base: float32 [2560], P('head'), may hold values from -1.5 to 1.5
- learning_down_matrix: bfloat16 [2560, 96], replicated, may hold values from -0.125 to 0.125
- learning_up_matrix: bfloat16 [96, 2560], P(None, 'head'), may hold values from -0.625 to 0.625
- key_scale: float32 [2560], P('head'), may hold values from 0.25 to 1.75
- key_blend: float32 [2560], P('head'), may hold values from 0.2 to 1
- norm_gain: float32 [2560], P('head'), may hold values from 0.25 to 1.75
- norm_bias: float32 [2560], P('head'), may hold values from -3 to 3
- output_weight: bfloat16 [2560, 2560], P('head'), may hold values from -0.125 to 0.125
Outputs:
- mixed_out: bfloat16 [2, 4096, 2560], P(None, 'seq', 'head')
The draws below stay inside these ranges and needn't reach their ends.
All inputs are finite; a program needn't handle non-finite values.
Results may differ from the reference program's by a relative error of at most 0.014.
Values may be sent and summed in bfloat16 or wider, within the bound.
No kernel may reach another device: no remote copies, remote signals or barrier semaphores. Data moves between devices by JAX's collectives and lax.ppermute only.
A program may use at most 128 MiB of HBM per device.

```python
import math
import jax
import jax.numpy as jnp
from jax import lax

MODEL_WIDTH = 2560
LOW_RANK_WIDTH = 96
HEAD_SIZE = 64
SEQS = 2
LENGTH = 4096


def draw_decay_base(key, part):
    first, second = jax.random.split(jax.random.fold_in(key, 17))
    fast_share = 0.5
    fast = jax.random.bernoulli(first, fast_share, (MODEL_WIDTH,))
    spread = jax.random.uniform(second, (MODEL_WIDTH,), jnp.float32)
    fast_low = math.log(1.0 / 48.0)
    fast_high = math.log(1.0 / 12.0)
    slow_low = math.log(0.2 / LENGTH)
    slow_high = math.log(1.0 / LENGTH)
    rates = jnp.where(fast, fast_low + spread * (fast_high - fast_low), slow_low + spread * (slow_high - slow_low))
    return (rates + 0.5).astype(jnp.float32)


def level_of(stream_key, dims, shards, low, largest):
    def one(position, shards_of):
        draws = jax.random.uniform(jax.random.fold_in(jax.random.fold_in(stream_key, 6), position), (shards_of,), jnp.float32, low / len(shards), largest / len(shards))
        return jnp.repeat(jnp.exp(draws), dims[position] // shards_of).reshape((-1,) + (1,) * (len(dims) - position - 1))

    gain = one(*shards[0])
    for cut in shards[1:]:
        gain = gain * one(*cut)
    return gain


def bell_draw(rng, dims, scale, bound, shards=(), kind=jnp.bfloat16):
    level = level_of(rng, dims, shards, -0.22, 0.18) if shards else 1.0
    array = jax.random.normal(rng, dims, jnp.float32) * scale * level
    return jnp.minimum(jnp.maximum(array, -bound), bound).astype(kind)


def setup_inputs(seed: int = 0) -> dict:
    streams_of = jax.random.split(jax.random.key(seed), 17)
    return {
        "tokens": bell_draw(streams_of[0], (SEQS, LENGTH, MODEL_WIDTH), 1.0, 6.0, ((1, 32), (2, 8))),
        "token_mix": jnp.clip(jax.random.uniform(streams_of[1], (5, MODEL_WIDTH), jnp.float32, 0.05, 0.95), 0.05, 0.95),
        "receptance": bell_draw(streams_of[2], (MODEL_WIDTH, MODEL_WIDTH), MODEL_WIDTH ** -0.5, 0.125, ((1, 8),)),
        "key_weight": bell_draw(streams_of[3], (MODEL_WIDTH, MODEL_WIDTH), MODEL_WIDTH ** -0.5, 0.125, ((1, 8),)),
        "value_weight": bell_draw(streams_of[4], (MODEL_WIDTH, MODEL_WIDTH), MODEL_WIDTH ** -0.5, 0.125, ((1, 8),)),
        "decay_base": draw_decay_base(jax.random.fold_in(streams_of[16], 71), 0),
        "decay_down_matrix": bell_draw(streams_of[6], (MODEL_WIDTH, LOW_RANK_WIDTH), MODEL_WIDTH ** -0.5, 0.125),
        "decay_up_matrix": bell_draw(streams_of[7], (LOW_RANK_WIDTH, MODEL_WIDTH), LOW_RANK_WIDTH ** -0.5, 0.625, ((1, 8),)),
        "learn_base": jnp.clip(jax.random.uniform(streams_of[8], (MODEL_WIDTH,), jnp.float32, -1.5, 1.5) * level_of(streams_of[8], (MODEL_WIDTH,), ((0, 8),), -0.4, 0.0), -1.5, 1.5),
        "learning_down_matrix": bell_draw(streams_of[9], (MODEL_WIDTH, LOW_RANK_WIDTH), MODEL_WIDTH ** -0.5, 0.125),
        "learning_up_matrix": bell_draw(streams_of[10], (LOW_RANK_WIDTH, MODEL_WIDTH), LOW_RANK_WIDTH ** -0.5, 0.625, ((1, 8),)),
        "key_scale": jnp.clip(1.0 + 0.15 * jax.random.normal(streams_of[11], (MODEL_WIDTH,), jnp.float32), 0.25, 1.75),
        "key_blend": jnp.clip(0.2 + 0.8 * jax.random.uniform(streams_of[12], (MODEL_WIDTH,), jnp.float32) ** level_of(streams_of[12], (MODEL_WIDTH,), ((0, 8),), -0.2, 0.2), 0.2, 1.0),
        "norm_gain": jnp.clip(1.0 + 0.15 * jax.random.normal(streams_of[13], (MODEL_WIDTH,), jnp.float32), 0.25, 1.75),
        "norm_bias": bell_draw(streams_of[14], (MODEL_WIDTH,), 0.5, 3.0, ((0, 8),), jnp.float32),
        "output_weight": bell_draw(streams_of[15], (MODEL_WIDTH, MODEL_WIDTH), MODEL_WIDTH ** -0.5, 0.125, ((0, 8),)),
    }


def reference(tokens, token_mix, receptance, key_weight, value_weight, decay_base, decay_down_matrix, decay_up_matrix, learn_base, learning_down_matrix, learning_up_matrix, key_scale, key_blend, norm_gain, norm_bias, output_weight):
    seq_count, length, width = tokens.shape
    head_count = width // HEAD_SIZE
    row_count = seq_count * length
    current = tokens.astype(jnp.float32)
    earlier = jnp.concatenate([jnp.zeros((seq_count, 1, width), jnp.float32), current[:, :-1]], axis=1)
    change = earlier - current

    def blended(which):
        return (current + change * token_mix[which]).astype(jnp.bfloat16).reshape(row_count, width)

    def product(left, right):
        return jnp.dot(left, right, preferred_element_type=jnp.float32)
    recept_out = product(blended(0), receptance)
    key_raw = product(blended(2), key_weight)
    value_out = product(blended(3), value_weight)
    decay_hidden = jnp.tanh(product(blended(1), decay_down_matrix)).astype(jnp.bfloat16)
    learn_hidden = product(blended(4), learning_down_matrix).astype(jnp.bfloat16)
    decay_arg = decay_base + product(decay_hidden, decay_up_matrix)
    log_decay = -jnp.exp(-jax.nn.softplus(-decay_arg) - 0.5)
    learn_rate = jax.nn.sigmoid(learn_base + product(learn_hidden, learning_up_matrix))
    scaled = (key_raw * key_scale).reshape(row_count, head_count, HEAD_SIZE)
    unit_key = (scaled / jnp.sqrt(lax.optimization_barrier(jnp.sum(scaled * scaled, axis=-1, keepdims=True)) + 1e-06)).reshape(row_count, width)
    key_final = key_raw * (1.0 + (learn_rate - 1.0) * key_blend)

    def arrange(values):
        return values.reshape(seq_count, length, head_count, HEAD_SIZE).transpose(1, 0, 2, 3)

    def advance(state, item):
        recept_t, decay_t, unit_t, learn_t, key_t, value_t = item
        drained = jnp.einsum('shvk,shk->shv', state, -unit_t, precision=lax.Precision.HIGHEST)
        state = state * jnp.exp(decay_t)[:, :, None, :] + drained[..., None] * (unit_t * learn_t)[:, :, None, :] + value_t[..., None] * key_t[:, :, None, :]
        return (state, jnp.einsum('shvk,shk->shv', state, recept_t, precision=lax.Precision.HIGHEST))
    start = jnp.zeros((seq_count, head_count, HEAD_SIZE, HEAD_SIZE), jnp.float32)
    items = (arrange(recept_out), arrange(log_decay), arrange(unit_key), arrange(learn_rate), arrange(key_final), arrange(value_out))
    final_state, outputs = lax.scan(advance, start, items)
    wkv = outputs.transpose(1, 0, 2, 3).reshape(row_count, head_count, HEAD_SIZE)
    centred = wkv - lax.optimization_barrier(jnp.mean(wkv, axis=-1, keepdims=True))
    spread = lax.optimization_barrier(jnp.mean(centred * centred, axis=-1, keepdims=True))
    normed = (centred / jnp.sqrt(spread + 0.00064)).reshape(row_count, width) * norm_gain + norm_bias
    normed = normed.astype(jnp.bfloat16)
    result = product(normed, output_weight).astype(jnp.bfloat16)
    return result.reshape(seq_count, length, width)
```

```python
import functools
import jax
import jax.numpy as jnp
from jax import lax
from jax.experimental import pallas as pl
from jax.experimental.pallas import tpu as pltpu
from jax.sharding import Mesh
from jax.sharding import PartitionSpec as P

HEAD = 64
SPAN = 64
SEQ = ("seq_0", "seq_1")
BF = jnp.bfloat16
F32 = jnp.float32
WORK = 2
VM = pl.BlockSpec(memory_space=pltpu.VMEM)
SM = pl.BlockSpec(memory_space=pltpu.SMEM)


def mm(a, b, ca=1, cb=0):
    return lax.dot_general(a, b, (((ca,), (cb,)), ((), ())), preferred_element_type=F32)


def split3(a):
    hi = a.astype(BF)
    rest = a - hi.astype(F32)
    mid = rest.astype(BF)
    low = (rest - mid.astype(F32)).astype(BF)
    return hi, mid, low


def head_ones(width):
    i = lax.broadcasted_iota(jnp.int32, (width, width), 0) // HEAD
    j = lax.broadcasted_iota(jnp.int32, (width, width), 1) // HEAD
    return (i == j).astype(F32).astype(BF)


def head_sums(a):
    hi, mid, low = split3(a)
    ones = head_ones(a.shape[1])
    return mm(hi, ones) + mm(mid, ones) + mm(low, ones)


def local_kernel(seqs, length, width, *refs):
    (order, p0, p1, p2, p3, p4, p5, p6, p7, near, far, mix, wr, wk, wv, wd, wl, base_d, up_d, base_l, up_l,
     scale, blend, maps_ref, query_ref, local_ref, accr, acck, accv, accd, accl) = refs
    pieces = (p0, p1, p2, p3, p4, p5, p6, p7)
    rows = seqs * length
    heads = width // HEAD
    spans = length // SPAN
    accs = (accr, accd, acck, accv, accl)
    weights = (wr, wd, wk, wv, wl)
    at = lax.broadcasted_iota(jnp.int32, (rows, width), 0)
    for k, piece in enumerate(pieces):
        cur = piece[...].astype(F32).reshape(rows, width)
        edges = near if k < 4 else far
        prev = pltpu.roll(cur, 1, 0)
        for s in range(seqs):
            row = edges[k % 4, s : s + 1, :].astype(F32)
            prev = jnp.where(at == s * length, row, prev)
        change = prev - cur
        where = order[k]
        m = mix[where]
        start = pl.multiple_of(where * width, 64)
        for j in range(5):
            b = (cur + change * m[j : j + 1, :]).astype(BF)
            out = mm(b, weights[j][pl.ds(start, width), :])
            if k == 0:
                accs[j][...] = out
            else:
                accs[j][...] += out
    recept = accr[...]
    key_raw = acck[...]
    value = accv[...]
    hidden_d = jnp.tanh(accd[...]).astype(BF)
    hidden_l = accl[...].astype(BF)
    arg_d = base_d[...] + mm(hidden_d, up_d[...])
    decay = -(jax.nn.sigmoid(arg_d) * 0.6065306597126334)
    rate = jax.nn.sigmoid(base_l[...] + mm(hidden_l, up_l[...]))
    scaled = key_raw * scale[...]
    unit = scaled * lax.rsqrt(head_sums(scaled * scaled) + 1e-06)
    key = key_raw * (1.0 + (rate - 1.0) * blend[...])
    ri = lax.broadcasted_iota(jnp.int32, (rows, rows), 0)
    ci = lax.broadcasted_iota(jnp.int32, (rows, rows), 1)
    tri = ((ri // SPAN == ci // SPAN) & (ri >= ci)).astype(F32).astype(BF)
    d_hi, d_mid, d_low = split3(decay)
    cumul = mm(tri, d_hi) + mm(tri, d_mid) + mm(tri, d_low)
    groups = rows // SPAN
    c3 = cumul.reshape(groups, SPAN, width)
    middle = c3[:, SPAN // 2 - 1 : SPAN // 2, :]
    ending = c3[:, SPAN - 1 :, :]
    rel = (c3 - middle).reshape(rows, width)
    e_mid = jnp.exp(middle)
    e_end = jnp.exp(ending)
    e_tail = jnp.exp(ending - middle)
    grow = jnp.exp(rel)
    shrink = jnp.exp(-rel)

    def spread(small, a):
        return (a.reshape(groups, SPAN, width) * small).reshape(rows, width)

    l_alpha = -unit * jnp.exp(rel - decay)
    l_recept = recept * grow
    r_beta = unit * rate * shrink
    r_key = key * shrink
    beta_end = spread(e_tail, r_beta)
    key_end = spread(e_tail, r_key)
    alpha_dec = spread(e_mid, l_alpha)
    recept_dec = spread(e_mid, l_recept)
    la, lr, rb, rk, vb = (a.astype(BF) for a in (l_alpha, l_recept, r_beta, r_key, value))
    gi = lax.broadcasted_iota(jnp.int32, (2 * SPAN, 2 * SPAN), 0)
    gj = lax.broadcasted_iota(jnp.int32, (2 * SPAN, 2 * SPAN), 1)
    keep = (gi % SPAN > gj % SPAN) | ((gi >= SPAN) & (gi % SPAN == gj % SPAN))
    eye = lax.broadcasted_iota(jnp.int32, (HEAD, HEAD), 0) == lax.broadcasted_iota(jnp.int32, (HEAD, HEAD), 1)
    units = [(s, h, c) for s in range(seqs) for h in range(heads) for c in range(spans)]

    def cut(a, u):
        s, h, c = u
        r0 = s * length + c * SPAN
        return a[r0 : r0 + SPAN, h * HEAD : (h + 1) * HEAD]

    powers, sols, outs, values = [], [], [], []
    for u in units:
        left = jnp.concatenate([cut(la, u), cut(lr, u)], axis=0)
        right = jnp.concatenate([cut(rb, u), cut(rk, u)], axis=0)
        g = jnp.where(keep, mm(left, right, 1, 1), 0.0).astype(BF)
        v = cut(vb, u)
        powers.append(g[:SPAN, :SPAN])
        outs.append(g[SPAN:, :])
        values.append(v)
        sols.append(jnp.concatenate([cut(alpha_dec, u), mm(g[:SPAN, SPAN:], v)], axis=1))
    levels = SPAN.bit_length() - 1
    for level in range(levels):
        for i in range(len(units)):
            if level < levels - 1:
                both = jnp.concatenate([sols[i].astype(BF), powers[i]], axis=1)
                y = mm(powers[i], both)
                sols[i] = sols[i] + y[:, : 2 * HEAD]
                powers[i] = y[:, 2 * HEAD :].astype(BF)
            else:
                sols[i] = sols[i] + mm(powers[i], sols[i].astype(BF))
    moves = []
    for i, u in enumerate(units):
        s, h, c = u
        v = values[i]
        rhs = jnp.concatenate([sols[i].astype(BF), jnp.concatenate([jnp.zeros_like(v), v], axis=1)], axis=0)
        ends = jnp.concatenate([cut(beta_end, u), cut(key_end, u)], axis=0)
        lhs = jnp.concatenate([outs[i], jnp.transpose(ends).astype(BF)], axis=0)
        y = mm(lhs, rhs)
        query = cut(recept_dec, u) + y[:SPAN, :HEAD]
        local = y[:SPAN, HEAD:]
        last = e_end[s * spans + c, :, h * HEAD : (h + 1) * HEAD]
        trans = y[SPAN:, :HEAD] + jnp.where(eye, last, 0.0)
        moves.append((query, local, trans, y[SPAN:, HEAD:]))
    half = HEAD // WORK
    for p in range(seqs * heads):
        q0, l0, t0, n0 = moves[2 * p]
        q1, l1, t1, n1 = moves[2 * p + 1]
        first = jnp.concatenate([t0, n0], axis=1).astype(BF)
        y = mm(jnp.concatenate([q1, t1], axis=0).astype(BF), first)
        query_ref[p, 0:SPAN, :] = q0.astype(BF)
        query_ref[p, SPAN:, :] = y[:SPAN, :HEAD].astype(BF)
        local_ref[p, 0:SPAN, :] = l0
        local_ref[p, SPAN:, :] = y[:SPAN, HEAD:] + l1
        trans = y[SPAN:, :HEAD] - jnp.where(eye, 1.0, 0.0)
        incr = y[SPAN:, HEAD:] + n1
        packed = jnp.concatenate([trans[:32], trans[32:]], axis=1).astype(BF)
        for w in range(WORK):
            part = incr[:, w * half : (w + 1) * half]
            block = jnp.concatenate([part[16 * i : 16 * i + 16] for i in range(4)], axis=1).astype(BF)
            maps_ref[p * WORK + w, 0:32, :] = packed
            maps_ref[p * WORK + w, 32:48, :] = block
    for w in range(seqs * heads * WORK, maps_ref.shape[0]):
        maps_ref[w] = jnp.zeros(maps_ref.shape[1:], BF)


def prefix_kernel(maps_ref, states_ref):
    steps = maps_ref.shape[0]
    group = 8
    groups = steps // group
    half = HEAD // WORK
    eye = (
        lax.broadcasted_iota(jnp.int32, (HEAD, HEAD), 0) == lax.broadcasted_iota(jnp.int32, (HEAD, HEAD), 1)
    ).astype(F32)
    start = jnp.concatenate([eye, jnp.zeros((HEAD, half), F32)], axis=1)

    def load(i):
        packed = maps_ref[i, 0:32, :]
        trans = jnp.concatenate([packed[:, :HEAD], packed[:, HEAD:]], axis=0)
        block = maps_ref[i, 32:48, :]
        incr = jnp.concatenate([block[:, 32 * j : 32 * j + 32] for j in range(4)], axis=0).astype(F32)
        return trans, incr

    run = [start] * groups
    seen = {}
    for i in range(group):
        for g in range(groups):
            seen[g, i] = run[g]
            trans, incr = load(g * group + i)
            add = mm(trans, run[g].astype(BF))
            run[g] = run[g] + add + jnp.concatenate([jnp.zeros((HEAD, HEAD), F32), incr], axis=1)
    state = jnp.zeros((HEAD, half), F32)
    for g in range(groups):
        sb = state.astype(BF)
        for i in range(group):
            a = seen[g, i]
            if i == 0:
                here = state
            else:
                here = state + mm((a[:, :HEAD] - eye).astype(BF), sb) + a[:, HEAD:]
            states_ref[g * group + i] = jnp.concatenate([here[16 * j : 16 * j + 16] for j in range(4)], axis=1).astype(BF)
        state = state + mm((run[g][:, :HEAD] - eye).astype(BF), sb) + run[g][:, HEAD:]


def norm_kernel(seqs, length, width, core, states_ref, query_ref, local_ref, gain, bias, w_out, keep_ref, send_ref):
    heads = width // HEAD
    for s in range(seqs):
        cols = []
        for h in range(heads):
            p = s * heads + h
            halves = []
            for w in range(WORK):
                block = states_ref[p * WORK + w]
                halves.append(jnp.concatenate([block[:, 32 * j : 32 * j + 32] for j in range(4)], axis=0))
            state = jnp.concatenate(halves, axis=1)
            out = mm(query_ref[p], state) + local_ref[p]
            centred = out - jnp.mean(out, axis=1, keepdims=True)
            spread = jnp.mean(centred * centred, axis=1, keepdims=True)
            cols.append(centred * lax.rsqrt(spread + 0.00064))
        normed = (jnp.concatenate(cols, axis=1) * gain[...] + bias[...]).astype(BF)

        @pl.when(core[0] == s)
        def _():
            keep_ref[...] = normed

        @pl.when(core[0] != s)
        def _():
            send_ref[...] = mm(normed, w_out[...]).astype(BF)


def sum_kernel(width, where, keep_ref, got_ref, w_out, own_ref, *sends):
    wide = 2 * width
    x = where[0]
    for i, out in enumerate((own_ref,) + sends):
        block = lax.rem(x + i, 4)
        cols = pl.ds(pl.multiple_of(block * wide, 128), wide)
        total = mm(keep_ref[...], w_out[:, cols]) + got_ref[:, cols].astype(F32)
        out[...] = total.astype(out.dtype)


def fold_kernel(width, core, own_ref, a_ref, b_ref, c_ref, mine_ref, give_ref):
    total = own_ref[...] + a_ref[...].astype(F32) + b_ref[...].astype(F32) + c_ref[...].astype(F32)
    low, high = total[:, :width].astype(BF), total[:, width:].astype(BF)

    @pl.when(core[0] == 0)
    def _():
        mine_ref[...] = low
        give_ref[...] = high

    @pl.when(core[0] != 0)
    def _():
        mine_ref[...] = high
        give_ref[...] = low


def place_kernel(core, mine_ref, got_ref, out_ref):
    out_ref[core[0]] = mine_ref[...]
    out_ref[1 - core[0]] = got_ref[...]


def body(
    tokens,
    token_mix,
    receptance,
    key_weight,
    value_weight,
    decay_base,
    decay_down_matrix,
    decay_up_matrix,
    learn_base,
    learning_down_matrix,
    learning_up_matrix,
    key_scale,
    key_blend,
    norm_gain,
    norm_bias,
    output_weight,
):
    seqs, length, width = tokens.shape
    rows = seqs * length
    heads = width // HEAD
    n_head = lax.axis_size("head")
    n_seq = lax.axis_size("seq_0") * lax.axis_size("seq_1")
    me = lax.axis_index("head")
    core = lax.rem(me, 2)
    core_s = core.reshape(1).astype(jnp.int32)
    x_s = (me // 2).reshape(1).astype(jnp.int32)

    def turn(v, d):
        return lax.ppermute(v, "head", [(i, (i + d) % n_head) for i in range(n_head)])

    def swap(v):
        return lax.ppermute(v, "head", [(i, i ^ 1) for i in range(n_head)])

    near = [tokens] + [turn(tokens, d) for d in (2, 4, 6)]
    far = [swap(a) for a in near]
    last = jnp.stack([a[:, length - 1, :] for a in near])
    edge_near = lax.ppermute(last, SEQ, [(i, i + 1) for i in range(n_seq - 1)])
    edge_far = swap(edge_near)
    offsets = jnp.array([0, 6, 4, 2], jnp.int32)
    order = jnp.concatenate([lax.rem(me + offsets, n_head), lax.rem((me ^ 1) + offsets, n_head)]).astype(jnp.int32)
    mix = jnp.transpose(token_mix.reshape(5, n_head, width), (1, 0, 2))
    row = lambda a: a.reshape(1, width)
    pairs = seqs * heads
    low = decay_down_matrix.shape[1]
    maps, query, local = pl.pallas_call(
        functools.partial(local_kernel, seqs, length, width),
        out_shape=[
            jax.ShapeDtypeStruct((n_seq, 48, 128), BF),
            jax.ShapeDtypeStruct((pairs, length, HEAD), BF),
            jax.ShapeDtypeStruct((pairs, length, HEAD), F32),
        ],
        in_specs=[SM] + [VM] * 22,
        out_specs=[VM] * 3,
        scratch_shapes=[pltpu.VMEM((rows, width), F32)] * 3 + [pltpu.VMEM((rows, low), F32)] * 2,
        name="local",
    )(
        order, *near, *far, edge_near, edge_far, mix, receptance, key_weight, value_weight,
        decay_down_matrix, learning_down_matrix, row(decay_base), decay_up_matrix, row(learn_base),
        learning_up_matrix, row(key_scale), row(key_blend),
    )
    got = lax.all_to_all(maps, SEQ, split_axis=0, concat_axis=0, tiled=True)
    states = pl.pallas_call(
        prefix_kernel,
        out_shape=jax.ShapeDtypeStruct((n_seq, 16, 128), BF),
        in_specs=[VM],
        out_specs=VM,
        name="prefix",
    )(got)
    states = lax.all_to_all(states, SEQ, split_axis=0, concat_axis=0, tiled=True)
    full = output_weight.shape[1]
    keep, send = pl.pallas_call(
        functools.partial(norm_kernel, seqs, length, width),
        out_shape=[jax.ShapeDtypeStruct((length, width), BF), jax.ShapeDtypeStruct((length, full), BF)],
        in_specs=[SM] + [VM] * 6,
        out_specs=[VM] * 2,
        name="norm",
    )(core_s, states, query, local, row(norm_gain), row(norm_bias), output_weight)
    half = swap(send)
    wide = 2 * width
    own, s1, s2, s3 = pl.pallas_call(
        functools.partial(sum_kernel, width),
        out_shape=[jax.ShapeDtypeStruct((length, wide), F32)] + [jax.ShapeDtypeStruct((length, wide), BF)] * 3,
        in_specs=[SM] + [VM] * 3,
        out_specs=[VM] * 4,
        name="partial",
    )(x_s, keep, half, output_weight)
    parts = [turn(s1, 2), turn(s2, 4), turn(s3, 6)]
    mine, give = pl.pallas_call(
        functools.partial(fold_kernel, width),
        out_shape=[jax.ShapeDtypeStruct((length, width), BF)] * 2,
        in_specs=[SM] + [VM] * 4,
        out_specs=[VM] * 2,
        name="fold",
    )(core_s, own, *parts)
    other = swap(give)
    return pl.pallas_call(
        place_kernel,
        out_shape=jax.ShapeDtypeStruct((seqs, length, width), BF),
        in_specs=[SM] + [VM] * 2,
        out_specs=VM,
        name="place",
    )(core_s, mine, other)


def solution(mesh):
    torus = Mesh(mesh.devices.reshape(4, 8, mesh.shape["head"]), ("seq_0", "seq_1", "head"))
    placed = (
        P(None, SEQ, "head"),
        P(),
        P(None, "head"),
        P(None, "head"),
        P(None, "head"),
        P("head"),
        P(),
        P(None, "head"),
        P("head"),
        P(),
        P(None, "head"),
        P("head"),
        P("head"),
        P("head"),
        P("head"),
        P("head", None),
    )
    return jax.shard_map(
        body, mesh=torus, in_specs=placed, out_specs=P(None, SEQ, "head"), check_vma=False
    )
```

```python
import functools
import jax
import jax.numpy as jnp
from jax import lax
from jax.experimental import pallas as pl
from jax.experimental.pallas import tpu as pltpu
from jax.sharding import Mesh
from jax.sharding import PartitionSpec as P

HEAD = 64
SPAN = 64
SEQ = ("seq_0", "seq_1")
BF = jnp.bfloat16
F32 = jnp.float32
WORK = 2
VM = pl.BlockSpec(memory_space=pltpu.VMEM)
SMALL = pltpu.CompilerParams(vmem_limit_bytes=20 * 1024 * 1024)


def mm(a, b, ca=1, cb=0):
    return lax.dot_general(a, b, (((ca,), (cb,)), ((), ())), preferred_element_type=F32)


def split3(a):
    hi = a.astype(BF)
    rest = a - hi.astype(F32)
    mid = rest.astype(BF)
    low = (rest - mid.astype(F32)).astype(BF)
    return hi, mid, low


def local_kernel(seqs, length, width, n_head, *refs):
    (p0, p1, p2, p3, p4, p5, p6, p7, near, far, mix, wr, wk, wv, wd, wl, up_d, up_l, *vecs) = refs[:22]
    (maps_ref, query_ref, local_ref, xs, vr, vk, vv, vd, vl, sems, mcol,
     la_s, lr_s, rb_s, rk_s, vb_s, be_s, ke_s, ad_s, rd_s, ee_s) = refs[22:]
    pieces = (p0, p1, p2, p3, p4, p5, p6, p7)
    copies = [
        pltpu.make_async_copy(a, b, sems.at[i])
        for i, (a, b) in enumerate(((wr, vr), (wd, vd), (wk, vk), (wv, vv), (wl, vl)))
    ]
    for c in copies:
        c.start()
    cols = seqs * length
    heads = width // HEAD
    me = lax.axis_index("head")
    mate = me + 1 - 2 * lax.rem(me, 2)
    steps = (0, 4, 6, 2)
    mix_rows = jnp.concatenate([mix[...], jnp.zeros((3, mix.shape[1]), F32)], axis=0)
    mcol[...] = jnp.transpose(mix_rows)
    edge_cols = jnp.transpose(jnp.concatenate([near[...], far[...]], axis=0).astype(F32))
    block = 64
    lane = lax.broadcasted_iota(jnp.int32, (block, length), 1)
    for k, piece in enumerate(pieces):
        owner = lax.rem((me if k < 4 else mate) + steps[k % 4], n_head)
        for q in range(width // block):
            start = pl.multiple_of(owner * width + q * block, block)
            m = mcol[pl.ds(start, block), :]
            for s in range(seqs):
                cur = piece[s, q * block : (q + 1) * block, :].astype(F32)
                r = k * seqs + s
                edge = edge_cols[q * block : (q + 1) * block, r : r + 1]
                prev = jnp.where(lane == 0, edge, pltpu.roll(cur, 1, 1))
                change = prev - cur
                for j in range(5):
                    xs[j, pl.ds(start, block), s * length : (s + 1) * length] = (
                        cur + change * m[:, j : j + 1]
                    ).astype(BF)
    copies[0].wait()
    recept = mm(vr[...], xs[0])
    copies[1].wait()
    hidden_d = jnp.tanh(mm(vd[...], xs[1])).astype(BF)
    copies[2].wait()
    key_raw = mm(vk[...], xs[2])
    copies[3].wait()
    vb_s[...] = mm(vv[...], xs[3]).astype(BF)
    copies[4].wait()
    hidden_l = mm(vl[...], xs[4]).astype(BF)
    vec_cols = jnp.transpose(jnp.concatenate([v[...].reshape(1, width) for v in vecs] * 2, axis=0))
    vec = lambda i: vec_cols[:, i : i + 1]
    decay = jax.nn.sigmoid(vec(0) + mm(up_d[...], hidden_d, 0, 0)) * (-0.6065306597126334)
    rate = jax.nn.sigmoid(vec(1) + mm(up_l[...], hidden_l, 0, 0))
    scaled = (key_raw * vec(2)).reshape(heads, HEAD, cols)
    unit = (scaled * lax.rsqrt(jnp.sum(scaled * scaled, axis=1, keepdims=True) + 1e-06)).reshape(width, cols)
    key = key_raw * (1.0 + (rate - 1.0) * vec(3))
    si = lax.broadcasted_iota(jnp.int32, (cols, cols), 0)
    ti = lax.broadcasted_iota(jnp.int32, (cols, cols), 1)
    same = si // SPAN == ti // SPAN
    one = lambda c: c.astype(F32)
    upto = one(same & (si <= ti))
    mid = one(same & (si % SPAN < SPAN // 2))
    parts = split3(decay)

    def summed(w):
        w = w.astype(BF)
        return mm(parts[0], w) + mm(parts[1], w) + mm(parts[2], w)

    rel = summed(upto - mid)
    e_mid = jnp.exp(summed(mid))
    e_tail = jnp.exp(summed(one(same) - mid))
    shrink = jnp.exp(-rel)
    l_alpha = -unit * jnp.exp(rel - decay)
    l_recept = recept * jnp.exp(rel)
    r_beta = unit * rate * shrink
    r_key = key * shrink
    be_s[...] = (e_tail * r_beta).astype(BF)
    ke_s[...] = (e_tail * r_key).astype(BF)
    ad_s[...] = e_mid * l_alpha
    rd_s[...] = e_mid * l_recept
    ee_s[...] = e_mid * e_tail
    la_s[...] = l_alpha.astype(BF)
    lr_s[...] = l_recept.astype(BF)
    rb_s[...] = r_beta.astype(BF)
    rk_s[...] = r_key.astype(BF)

    gs = lax.broadcasted_iota(jnp.int32, (2 * length, 2 * length), 0) % length
    gt0 = lax.broadcasted_iota(jnp.int32, (2 * length, 2 * length), 1)
    gt = gt0 % length
    keep = (gs // SPAN == gt // SPAN) & ((gs < gt) | ((gt0 >= length) & (gs == gt)))
    first_lane = lax.broadcasted_iota(jnp.int32, (HEAD, length), 1) < SPAN
    ei = lax.broadcasted_iota(jnp.int32, (HEAD, 2 * HEAD), 0)
    ej = lax.broadcasted_iota(jnp.int32, (HEAD, 2 * HEAD), 1)
    eye = ei == ej
    half = HEAD // WORK
    levels = SPAN.bit_length() - 1

    def per_seq(s, _):
        at = pl.ds(pl.multiple_of(s * length, length), length)

        def cut(a, h):
            return a[h * HEAD : (h + 1) * HEAD, at]

        powers, sols, outs, values = [], [], [], []
        for h in range(heads):
            right = jnp.concatenate([cut(rb_s, h), cut(rk_s, h)], axis=1)
            left = jnp.concatenate([cut(la_s, h), cut(lr_s, h)], axis=1)
            g = jnp.where(keep, mm(right, left, 0, 0), 0.0).astype(BF)
            v = cut(vb_s, h)
            powers.append(g[:length, :length])
            outs.append(g[:, length:])
            values.append(v)
            sols.append(jnp.concatenate([cut(ad_s, h), mm(v, g[length:, :length])], axis=0))
        for level in range(levels):
            for i in range(heads):
                if level < levels - 1:
                    both = jnp.concatenate([sols[i].astype(BF), powers[i]], axis=0)
                    y = mm(both, powers[i])
                    sols[i] = sols[i] + y[: 2 * HEAD]
                    powers[i] = y[2 * HEAD :].astype(BF)
                else:
                    sols[i] = sols[i] + mm(sols[i].astype(BF), powers[i])
        for h in range(heads):
            p = s * heads + h
            v = values[h]
            rhs = jnp.concatenate([sols[h].astype(BF), jnp.concatenate([jnp.zeros_like(v), v], axis=0)], axis=1)
            y = mm(rhs, outs[h])
            query = cut(rd_s, h) + y[:HEAD]
            local = y[HEAD:]
            be, ke = cut(be_s, h), cut(ke_s, h)
            zero = jnp.zeros_like(be)
            ends = jnp.concatenate(
                [
                    jnp.concatenate([jnp.where(first_lane, be, zero), jnp.where(first_lane, ke, zero)], axis=1),
                    jnp.concatenate([jnp.where(first_lane, zero, be), jnp.where(first_lane, zero, ke)], axis=1),
                ],
                axis=0,
            )
            y = mm(ends, rhs, 1, 1)
            last = cut(ee_s, h)
            m0 = (y[:HEAD] + jnp.where(eye, last[:, 0:1], 0.0)).astype(BF)
            m1 = y[HEAD:] + jnp.where(eye, last[:, SPAN : SPAN + 1], 0.0)
            y = mm(m1[:, :HEAD].astype(BF), m0)
            z = mm(m0, query.astype(BF), 0, 0)
            query_ref[p] = jnp.where(first_lane, query, z[:HEAD]).astype(BF)
            local_ref[p] = jnp.where(first_lane, local, local + z[HEAD:])
            total = y + jnp.where(ej >= HEAD, m1, 0.0) - jnp.where(eye, 1.0, 0.0)
            packed = jnp.concatenate([total[:32, :HEAD], total[32:, :HEAD]], axis=1).astype(BF)
            for w in range(WORK):
                part = total[:, HEAD + w * half : HEAD + (w + 1) * half]
                block = jnp.concatenate([part[16 * i : 16 * i + 16] for i in range(4)], axis=1).astype(BF)
                maps_ref[p * WORK + w, 0:32, :] = packed
                maps_ref[p * WORK + w, 32:48, :] = block
        return 0

    lax.fori_loop(0, seqs, per_seq, 0, unroll=True)
    for w in range(seqs * heads * WORK, maps_ref.shape[0]):
        maps_ref[w] = jnp.zeros(maps_ref.shape[1:], BF)


def call_local(near, far, edges, mix, wr, wk, wv, wd, wl, up_d, up_l, vecs, n_seq):
    seqs, width, length = near[0].shape
    n_head = len(near) + len(far)
    wide = n_head * width
    low = wd.shape[0]
    cols = seqs * length
    pairs = seqs * (width // HEAD)
    any_ = pl.BlockSpec(memory_space=pltpu.HBM)
    return pl.pallas_call(
        functools.partial(local_kernel, seqs, length, width, n_head),
        out_shape=[
            jax.ShapeDtypeStruct((n_seq, 48, 128), BF),
            jax.ShapeDtypeStruct((pairs, HEAD, length), BF),
            jax.ShapeDtypeStruct((pairs, HEAD, length), F32),
        ],
        in_specs=[VM] * 11 + [any_] * 5 + [VM] * 6,
        out_specs=[VM] * 3,
        scratch_shapes=[
            pltpu.VMEM((5, wide, cols), BF),
            *[pltpu.VMEM((width, wide), BF)] * 3,
            *[pltpu.VMEM((low, wide), BF)] * 2,
            pltpu.SemaphoreType.DMA((5,)),
            pltpu.VMEM((wide, 8), F32),
            *[pltpu.VMEM((width, cols), BF)] * 7,
            *[pltpu.VMEM((width, cols), F32)] * 3,
        ],
        compiler_params=pltpu.CompilerParams(vmem_limit_bytes=40 * 1024 * 1024),
        name="local",
    )(*near, *far, *edges, mix, wr, wk, wv, wd, wl, up_d, up_l, *vecs)


def prefix_kernel(maps_ref, states_ref):
    steps = maps_ref.shape[0]
    group = 8
    groups = steps // group
    half = HEAD // WORK
    eye = (
        lax.broadcasted_iota(jnp.int32, (HEAD, HEAD), 0) == lax.broadcasted_iota(jnp.int32, (HEAD, HEAD), 1)
    ).astype(F32)
    start = jnp.concatenate([eye, jnp.zeros((HEAD, half), F32)], axis=1)

    def load(i):
        packed = maps_ref[i, 0:32, :]
        trans = jnp.concatenate([packed[:, :HEAD], packed[:, HEAD:]], axis=0)
        block = maps_ref[i, 32:48, :]
        incr = jnp.concatenate([block[:, 32 * j : 32 * j + 32] for j in range(4)], axis=0).astype(F32)
        return trans, incr

    run = [start] * groups
    seen = {}
    for i in range(group):
        for g in range(groups):
            seen[g, i] = run[g]
            trans, incr = load(g * group + i)
            add = mm(trans, run[g].astype(BF))
            run[g] = run[g] + add + jnp.concatenate([jnp.zeros((HEAD, HEAD), F32), incr], axis=1)
    state = jnp.zeros((HEAD, half), F32)
    for g in range(groups):
        sb = state.astype(BF)
        for i in range(group):
            a = seen[g, i]
            if i == 0:
                here = state
            else:
                here = state + mm((a[:, :HEAD] - eye).astype(BF), sb) + a[:, HEAD:]
            states_ref[g * group + i] = jnp.concatenate([here[16 * j : 16 * j + 16] for j in range(4)], axis=1).astype(BF)
        state = state + mm((run[g][:, :HEAD] - eye).astype(BF), sb) + run[g][:, HEAD:]


def norm_kernel(seqs, width, states_ref, query_ref, local_ref, gain, bias, w_out, keep_ref, send_ref):
    heads = width // HEAD
    core = lax.rem(lax.axis_index("head"), 2)
    vec_cols = jnp.transpose(jnp.concatenate([v[...].reshape(1, width) for v in (gain, bias)] * 4, axis=0))
    for s in range(seqs):
        blocks = []
        for h in range(heads):
            p = s * heads + h
            halves = []
            for w in range(WORK):
                block = states_ref[p * WORK + w]
                halves.append(jnp.concatenate([block[:, 32 * j : 32 * j + 32] for j in range(4)], axis=0))
            state = jnp.concatenate(halves, axis=1)
            out = mm(state, query_ref[p], 0, 0) + local_ref[p]
            centred = out - jnp.mean(out, axis=0, keepdims=True)
            spread = jnp.mean(centred * centred, axis=0, keepdims=True)
            blocks.append(centred * lax.rsqrt(spread + 0.00064))
        normed = (jnp.concatenate(blocks, axis=0) * vec_cols[:, 0:1] + vec_cols[:, 1:2]).astype(BF)

        @pl.when(core == s)
        def _():
            keep_ref[...] = normed

        @pl.when(core != s)
        def _():
            send_ref[...] = mm(normed, w_out[...], 0, 0).astype(BF)


def sum_kernel(width, keep_ref, got_ref, w_out, *outs):
    wide = 2 * width
    me = lax.axis_index("head")
    x, c = me // 2, lax.rem(me, 2)
    for i in range(4):
        block = lax.rem(x + i, 4)
        cols = pl.ds(pl.multiple_of(block * wide, 128), wide)
        total = mm(keep_ref[...], w_out[:, cols], 0, 0) + got_ref[:, cols].astype(F32)
        low, high = total[:, :width], total[:, width:]
        same, cross = outs[2 * i], outs[2 * i + 1]
        same[...] = jnp.where(c == 0, low, high).astype(same.dtype)
        cross[...] = jnp.where(c == 0, high, low).astype(cross.dtype)


def fold_kernel(*refs):
    out_ref = refs[-1]
    c = lax.rem(lax.axis_index("head"), 2)
    for i, slot in ((0, c), (1, 1 - c)):
        total = refs[i][...].astype(F32)
        for k in (1, 2, 3):
            total = total + refs[2 * k + i][...].astype(F32)
        out_ref[slot] = jnp.transpose(total).astype(BF)


def body(
    tokens,
    token_mix,
    receptance,
    key_weight,
    value_weight,
    decay_base,
    decay_down_matrix,
    decay_up_matrix,
    learn_base,
    learning_down_matrix,
    learning_up_matrix,
    key_scale,
    key_blend,
    norm_gain,
    norm_bias,
    output_weight,
):
    seqs, length, width = tokens.shape
    n_head = lax.axis_size("head")
    n_seq = lax.axis_size("seq_0") * lax.axis_size("seq_1")

    def turn(v, d):
        return lax.ppermute(v, "head", [(i, (i + d) % n_head) for i in range(n_head)])

    def swap(v, d=0):
        return lax.ppermute(v, "head", [(i, ((i + d) % n_head) ^ 1) for i in range(n_head)])

    turned = jnp.transpose(tokens, (0, 2, 1))
    near = [turned] + [turn(turned, d) for d in (4, 2, 6)]
    far = [swap(a) for a in near]
    edge = lax.ppermute(tokens[:, length - 1, :], SEQ, [(i, i + 1) for i in range(n_seq - 1)])
    edge_near = jnp.concatenate([edge] + [turn(edge, d) for d in (4, 2, 6)], axis=0)
    edges = (edge_near, swap(edge_near))
    maps, query, local = call_local(
        near, far, edges, token_mix, receptance.T, key_weight.T, value_weight.T,
        decay_down_matrix.T, learning_down_matrix.T, decay_up_matrix, learning_up_matrix,
        (decay_base, learn_base, key_scale, key_blend), n_seq,
    )
    got = lax.all_to_all(maps, SEQ, split_axis=0, concat_axis=0, tiled=True)
    states = pl.pallas_call(
        prefix_kernel,
        out_shape=jax.ShapeDtypeStruct((n_seq, 16, 128), BF),
        in_specs=[VM],
        out_specs=VM,
        compiler_params=SMALL,
        name="prefix",
    )(got)
    states = lax.all_to_all(states, SEQ, split_axis=0, concat_axis=0, tiled=True)
    full = output_weight.shape[1]
    keep, send = pl.pallas_call(
        functools.partial(norm_kernel, seqs, width),
        out_shape=[jax.ShapeDtypeStruct((width, length), BF), jax.ShapeDtypeStruct((length, full), BF)],
        in_specs=[VM] * 6,
        out_specs=[VM] * 2,
        compiler_params=SMALL,
        name="norm",
    )(states, query, local, norm_gain, norm_bias, output_weight)
    half = swap(send)
    outs = pl.pallas_call(
        functools.partial(sum_kernel, width),
        out_shape=[jax.ShapeDtypeStruct((length, width), F32)] + [jax.ShapeDtypeStruct((length, width), BF)] * 7,
        in_specs=[VM] * 3,
        out_specs=[VM] * 8,
        compiler_params=SMALL,
        name="partial",
    )(keep, half, output_weight)
    parts = [outs[0], swap(outs[1])]
    for d in (1, 2, 3):
        parts += [turn(outs[2 * d], 2 * d), swap(outs[2 * d + 1], 2 * d)]
    out = pl.pallas_call(
        fold_kernel,
        out_shape=jax.ShapeDtypeStruct((seqs, width, length), BF),
        in_specs=[VM] * 8,
        out_specs=VM,
        compiler_params=SMALL,
        name="fold",
    )(*parts)
    return jnp.transpose(out, (0, 2, 1))


def solution(mesh):
    torus = Mesh(mesh.devices.reshape(4, 8, mesh.shape["head"]), ("seq_0", "seq_1", "head"))
    placed = (
        P(None, SEQ, "head"),
        P(),
        P(None, "head"),
        P(None, "head"),
        P(None, "head"),
        P("head"),
        P(),
        P(None, "head"),
        P("head"),
        P(),
        P(None, "head"),
        P("head"),
        P("head"),
        P("head"),
        P("head"),
        P("head", None),
    )
    return jax.shard_map(
        body, mesh=torus, in_specs=placed, out_specs=P(None, SEQ, "head"), check_vma=False
    )
```

```python
import functools
import jax
import jax.numpy as jnp
from jax import lax
from jax.experimental import pallas as pl
from jax.experimental.pallas import tpu as pltpu
from jax.sharding import Mesh
from jax.sharding import PartitionSpec as P

HEAD = 64
SPAN = 64
SEQ = ("seq_0", "seq_1")
BF = jnp.bfloat16
F32 = jnp.float32
EDGE = 32
WORK = 2
VM = pl.BlockSpec(memory_space=pltpu.VMEM)
SMALL = pltpu.CompilerParams(vmem_limit_bytes=20 * 1024 * 1024)


def mm(a, b, ca=1, cb=0):
    return lax.dot_general(a, b, (((ca,), (cb,)), ((), ())), preferred_element_type=F32)


def split3(a):
    hi = a.astype(BF)
    rest = a - hi.astype(F32)
    mid = rest.astype(BF)
    low = (rest - mid.astype(F32)).astype(BF)
    return hi, mid, low


def local_kernel(seqs, length, width, n_head, *refs):
    (p0, p1, p2, p3, p4, p5, p6, p7, near, far, mix, wr, wk, wv, wd, wl, up_d, up_l, *vecs) = refs[:22]
    (maps_ref, query_ref, local_ref, xs, vp, vr, vk, vv, vd, vl, vm, sems, mcol,
     la_s, lr_s, rb_s, rk_s, vb_s, be_s, ke_s, ad_s, rd_s, ee_s) = refs[22:]
    pieces = (p0, p1, p2, p3, p4, p5, p6, p7)
    moved = [(wr, vr), (wd, vd), (wk, vk), (wv, vv), (wl, vl), (mix, vm)] + [(p, vp.at[k]) for k, p in enumerate(pieces)]
    copies = [pltpu.make_async_copy(a, b, sems.at[i]) for i, (a, b) in enumerate(moved)]
    for c in copies[5:] + copies[:5]:
        c.start()
    cols = seqs * length
    heads = width // HEAD
    me = lax.axis_index("head")
    mate = me + 1 - 2 * lax.rem(me, 2)
    steps = (0, 4, 6, 2)
    edge_cols = jnp.transpose(jnp.concatenate([near[...], far[...]], axis=0).astype(F32))
    copies[5].wait()
    mcol[...] = jnp.transpose(jnp.concatenate([vm[...], jnp.zeros((3, vm.shape[1]), F32)], axis=0))
    block = 64
    lane = lax.broadcasted_iota(jnp.int32, (block, length), 1)
    for k in range(n_head):
        copies[6 + k].wait()
        owner = lax.rem((me if k < 4 else mate) + steps[k % 4], n_head)
        for q in range(width // block):
            start = pl.multiple_of(owner * width + q * block, block)
            m = mcol[pl.ds(start, block), :]
            for s in range(seqs):
                cur = vp[k, s, q * block : (q + 1) * block, :].astype(F32)
                f = s * width + q * block
                r = (k // 4) * EDGE + (k % 4) * 5 + f // 128
                edge = edge_cols[f % 128 : f % 128 + block, r : r + 1]
                prev = jnp.where(lane == 0, edge, pltpu.roll(cur, 1, 1))
                change = prev - cur
                for j in range(5):
                    xs[j, pl.ds(start, block), s * length : (s + 1) * length] = (
                        cur + change * m[:, j : j + 1]
                    ).astype(BF)
    copies[0].wait()
    recept = mm(vr[...], xs[0])
    copies[1].wait()
    hidden_d = jnp.tanh(mm(vd[...], xs[1])).astype(BF)
    copies[2].wait()
    key_raw = mm(vk[...], xs[2])
    copies[3].wait()
    vb_s[...] = mm(vv[...], xs[3]).astype(BF)
    copies[4].wait()
    hidden_l = mm(vl[...], xs[4]).astype(BF)
    vec_cols = jnp.transpose(jnp.concatenate([v[...].reshape(1, width) for v in vecs] * 2, axis=0))
    vec = lambda i: vec_cols[:, i : i + 1]
    decay = jax.nn.sigmoid(vec(0) + mm(up_d[...], hidden_d, 0, 0)) * (-0.6065306597126334)
    rate = jax.nn.sigmoid(vec(1) + mm(up_l[...], hidden_l, 0, 0))
    scaled = (key_raw * vec(2)).reshape(heads, HEAD, cols)
    unit = (scaled * lax.rsqrt(jnp.sum(scaled * scaled, axis=1, keepdims=True) + 1e-06)).reshape(width, cols)
    key = key_raw * (1.0 + (rate - 1.0) * vec(3))
    si = lax.broadcasted_iota(jnp.int32, (cols, cols), 0)
    ti = lax.broadcasted_iota(jnp.int32, (cols, cols), 1)
    same = si // SPAN == ti // SPAN
    one = lambda c: c.astype(F32)
    upto = one(same & (si <= ti))
    mid = one(same & (si % SPAN < SPAN // 2))
    parts = split3(decay)

    def summed(w):
        w = w.astype(BF)
        return mm(parts[0], w) + mm(parts[1], w) + mm(parts[2], w)

    rel = summed(upto - mid)
    e_mid = jnp.exp(summed(mid))
    e_tail = jnp.exp(summed(one(same) - mid))
    shrink = jnp.exp(-rel)
    l_alpha = -unit * jnp.exp(rel - decay)
    l_recept = recept * jnp.exp(rel)
    r_beta = unit * rate * shrink
    r_key = key * shrink
    be_s[...] = (e_tail * r_beta).astype(BF)
    ke_s[...] = (e_tail * r_key).astype(BF)
    ad_s[...] = e_mid * l_alpha
    rd_s[...] = e_mid * l_recept
    ee_s[...] = e_mid * e_tail
    la_s[...] = l_alpha.astype(BF)
    lr_s[...] = l_recept.astype(BF)
    rb_s[...] = r_beta.astype(BF)
    rk_s[...] = r_key.astype(BF)

    gs = lax.broadcasted_iota(jnp.int32, (2 * length, 2 * length), 0) % length
    gt0 = lax.broadcasted_iota(jnp.int32, (2 * length, 2 * length), 1)
    gt = gt0 % length
    keep = (gs // SPAN == gt // SPAN) & ((gs < gt) | ((gt0 >= length) & (gs == gt)))
    first_lane = lax.broadcasted_iota(jnp.int32, (HEAD, length), 1) < SPAN
    ei = lax.broadcasted_iota(jnp.int32, (HEAD, 2 * HEAD), 0)
    ej = lax.broadcasted_iota(jnp.int32, (HEAD, 2 * HEAD), 1)
    eye = ei == ej
    half = HEAD // WORK
    levels = SPAN.bit_length() - 1

    def per_seq(s, _):
        at = pl.ds(pl.multiple_of(s * length, length), length)

        def cut(a, h):
            return a[h * HEAD : (h + 1) * HEAD, at]

        powers, sols, outs, values = [], [], [], []
        for h in range(heads):
            right = jnp.concatenate([cut(rb_s, h), cut(rk_s, h)], axis=1)
            left = jnp.concatenate([cut(la_s, h), cut(lr_s, h)], axis=1)
            g = jnp.where(keep, mm(right, left, 0, 0), 0.0).astype(BF)
            v = cut(vb_s, h)
            powers.append(g[:length, :length])
            outs.append(g[:, length:])
            values.append(v)
            sols.append(jnp.concatenate([cut(ad_s, h), mm(v, g[length:, :length])], axis=0))
        for level in range(levels):
            for i in range(heads):
                if level < levels - 1:
                    both = jnp.concatenate([sols[i].astype(BF), powers[i]], axis=0)
                    y = mm(both, powers[i])
                    sols[i] = sols[i] + y[: 2 * HEAD]
                    powers[i] = y[2 * HEAD :].astype(BF)
                else:
                    sols[i] = sols[i] + mm(sols[i].astype(BF), powers[i])
        for h in range(heads):
            p = s * heads + h
            v = values[h]
            rhs = jnp.concatenate([sols[h].astype(BF), jnp.concatenate([jnp.zeros_like(v), v], axis=0)], axis=1)
            y = mm(rhs, outs[h])
            query = cut(rd_s, h) + y[:HEAD]
            local = y[HEAD:]
            be, ke = cut(be_s, h), cut(ke_s, h)
            zero = jnp.zeros_like(be)
            ends = jnp.concatenate(
                [
                    jnp.concatenate([jnp.where(first_lane, be, zero), jnp.where(first_lane, ke, zero)], axis=1),
                    jnp.concatenate([jnp.where(first_lane, zero, be), jnp.where(first_lane, zero, ke)], axis=1),
                ],
                axis=0,
            )
            y = mm(ends, rhs, 1, 1)
            last = cut(ee_s, h)
            m0 = (y[:HEAD] + jnp.where(eye, last[:, 0:1], 0.0)).astype(BF)
            m1 = y[HEAD:] + jnp.where(eye, last[:, SPAN : SPAN + 1], 0.0)
            y = mm(m1[:, :HEAD].astype(BF), m0)
            z = mm(m0, query.astype(BF), 0, 0)
            query_ref[p] = jnp.where(first_lane, query, z[:HEAD]).astype(BF)
            local_ref[p] = jnp.where(first_lane, local, local + z[HEAD:])
            total = y + jnp.where(ej >= HEAD, m1, 0.0) - jnp.where(eye, 1.0, 0.0)
            packed = jnp.concatenate([total[:32, :HEAD], total[32:, :HEAD]], axis=1).astype(BF)
            for w in range(WORK):
                part = total[:, HEAD + w * half : HEAD + (w + 1) * half]
                block = jnp.concatenate([part[16 * i : 16 * i + 16] for i in range(4)], axis=1).astype(BF)
                maps_ref[p * WORK + w, 0:32, :] = packed
                maps_ref[p * WORK + w, 32:48, :] = block
        return 0

    lax.fori_loop(0, seqs, per_seq, 0, unroll=True)
    for w in range(seqs * heads * WORK, maps_ref.shape[0]):
        maps_ref[w] = jnp.zeros(maps_ref.shape[1:], BF)


def edge_kernel(p0, p1, p2, p3, out_ref):
    rows = []
    for p in (p0, p1, p2, p3):
        seqs, width, length = p.shape
        for r in range(seqs * width // 128):
            parts = []
            for q in (0, 64):
                f = r * 128 + q
                parts.append(p[f // width, f % width : f % width + 64, :])
            rows.append(jnp.transpose(jnp.concatenate(parts, axis=0).astype(F32))[length - 1 :, :])
    rows.append(jnp.zeros((EDGE - len(rows), 128), F32))
    out_ref[...] = jnp.concatenate(rows, axis=0).astype(BF)


def call_local(near, far, edges, mix, wr, wk, wv, wd, wl, up_d, up_l, vecs, n_seq):
    seqs, width, length = near[0].shape
    n_head = len(near) + len(far)
    wide = n_head * width
    low = wd.shape[0]
    cols = seqs * length
    pairs = seqs * (width // HEAD)
    any_ = pl.BlockSpec(memory_space=pltpu.HBM)
    return pl.pallas_call(
        functools.partial(local_kernel, seqs, length, width, n_head),
        out_shape=[
            jax.ShapeDtypeStruct((n_seq, 48, 128), BF),
            jax.ShapeDtypeStruct((pairs, HEAD, length), BF),
            jax.ShapeDtypeStruct((pairs, HEAD, length), F32),
        ],
        in_specs=[any_] * 8 + [VM] * 2 + [any_] * 6 + [VM] * 6,
        out_specs=[VM] * 3,
        scratch_shapes=[
            pltpu.VMEM((5, wide, cols), BF),
            pltpu.VMEM((n_head, seqs, width, length), BF),
            *[pltpu.VMEM((width, wide), BF)] * 3,
            *[pltpu.VMEM((low, wide), BF)] * 2,
            pltpu.VMEM(mix.shape, F32),
            pltpu.SemaphoreType.DMA((14,)),
            pltpu.VMEM((wide, 8), F32),
            *[pltpu.VMEM((width, cols), BF)] * 7,
            *[pltpu.VMEM((width, cols), F32)] * 3,
        ],
        name="local",
    )(*near, *far, *edges, mix, wr, wk, wv, wd, wl, up_d, up_l, *vecs)


def prefix_kernel(maps_ref, states_ref):
    steps = maps_ref.shape[0]
    group = 8
    groups = steps // group
    half = HEAD // WORK
    eye = (
        lax.broadcasted_iota(jnp.int32, (HEAD, HEAD), 0) == lax.broadcasted_iota(jnp.int32, (HEAD, HEAD), 1)
    ).astype(F32)
    start = jnp.concatenate([eye, jnp.zeros((HEAD, half), F32)], axis=1)

    def load(i):
        packed = maps_ref[i, 0:32, :]
        trans = jnp.concatenate([packed[:, :HEAD], packed[:, HEAD:]], axis=0)
        block = maps_ref[i, 32:48, :]
        incr = jnp.concatenate([block[:, 32 * j : 32 * j + 32] for j in range(4)], axis=0).astype(F32)
        return trans, incr

    run = [start] * groups
    seen = {}
    for i in range(group):
        for g in range(groups):
            seen[g, i] = run[g]
            trans, incr = load(g * group + i)
            add = mm(trans, run[g].astype(BF))
            run[g] = run[g] + add + jnp.concatenate([jnp.zeros((HEAD, HEAD), F32), incr], axis=1)
    state = jnp.zeros((HEAD, half), F32)
    for g in range(groups):
        sb = state.astype(BF)
        for i in range(group):
            a = seen[g, i]
            if i == 0:
                here = state
            else:
                here = state + mm((a[:, :HEAD] - eye).astype(BF), sb) + a[:, HEAD:]
            states_ref[g * group + i] = jnp.concatenate([here[16 * j : 16 * j + 16] for j in range(4)], axis=1).astype(BF)
        state = state + mm((run[g][:, :HEAD] - eye).astype(BF), sb) + run[g][:, HEAD:]


def norm_kernel(seqs, width, states_ref, query_ref, local_ref, gain, bias, w_out, keep_ref, send_ref):
    heads = width // HEAD
    core = lax.rem(lax.axis_index("head"), 2)
    vec_cols = jnp.transpose(jnp.concatenate([v[...].reshape(1, width) for v in (gain, bias)] * 4, axis=0))
    for s in range(seqs):
        blocks = []
        for h in range(heads):
            p = s * heads + h
            halves = []
            for w in range(WORK):
                block = states_ref[p * WORK + w]
                halves.append(jnp.concatenate([block[:, 32 * j : 32 * j + 32] for j in range(4)], axis=0))
            state = jnp.concatenate(halves, axis=1)
            out = mm(state, query_ref[p], 0, 0) + local_ref[p]
            centred = out - jnp.mean(out, axis=0, keepdims=True)
            spread = jnp.mean(centred * centred, axis=0, keepdims=True)
            blocks.append(centred * lax.rsqrt(spread + 0.00064))
        normed = (jnp.concatenate(blocks, axis=0) * vec_cols[:, 0:1] + vec_cols[:, 1:2]).astype(BF)

        @pl.when(core == s)
        def _():
            keep_ref[...] = normed

        @pl.when(core != s)
        def _():
            send_ref[...] = mm(normed, w_out[...], 0, 0).astype(BF)


def sum_kernel(width, keep_ref, got_ref, w_out, *outs):
    wide = 2 * width
    me = lax.axis_index("head")
    x, c = me // 2, lax.rem(me, 2)
    for i in range(4):
        block = lax.rem(x + i, 4)
        cols = pl.ds(pl.multiple_of(block * wide, 128), wide)
        total = mm(keep_ref[...], w_out[:, cols], 0, 0) + got_ref[:, cols].astype(F32)
        low, high = total[:, :width], total[:, width:]
        same, cross = outs[2 * i], outs[2 * i + 1]
        same[...] = jnp.where(c == 0, low, high).astype(same.dtype)
        cross[...] = jnp.where(c == 0, high, low).astype(cross.dtype)


def fold_kernel(*refs):
    out_ref = refs[-1]
    c = lax.rem(lax.axis_index("head"), 2)
    for i, slot in ((0, c), (1, 1 - c)):
        total = refs[i][...].astype(F32)
        for k in (1, 2, 3):
            total = total + refs[2 * k + i][...].astype(F32)
        out_ref[slot] = jnp.transpose(total).astype(BF)


def body(
    tokens,
    token_mix,
    receptance,
    key_weight,
    value_weight,
    decay_base,
    decay_down_matrix,
    decay_up_matrix,
    learn_base,
    learning_down_matrix,
    learning_up_matrix,
    key_scale,
    key_blend,
    norm_gain,
    norm_bias,
    output_weight,
):
    seqs, length, width = tokens.shape
    n_head = lax.axis_size("head")
    n_seq = lax.axis_size("seq_0") * lax.axis_size("seq_1")

    def turn(v, d):
        return lax.ppermute(v, "head", [(i, (i + d) % n_head) for i in range(n_head)])

    def swap(v, d=0):
        return lax.ppermute(v, "head", [(i, ((i + d) % n_head) ^ 1) for i in range(n_head)])

    turned = jnp.transpose(tokens, (0, 2, 1))
    near = [turned] + [turn(turned, d) for d in (4, 2, 6)]
    far = [swap(a) for a in near]
    edge = pl.pallas_call(
        edge_kernel,
        out_shape=jax.ShapeDtypeStruct((EDGE, 128), BF),
        in_specs=[VM] * 4,
        out_specs=VM,
        compiler_params=SMALL,
        name="edge",
    )(*near)
    edge_near = lax.ppermute(edge, SEQ, [(i, i + 1) for i in range(n_seq - 1)])
    edges = (edge_near, swap(edge_near))
    maps, query, local = call_local(
        near, far, edges, token_mix, receptance.T, key_weight.T, value_weight.T,
        decay_down_matrix.T, learning_down_matrix.T, decay_up_matrix, learning_up_matrix,
        (decay_base, learn_base, key_scale, key_blend), n_seq,
    )
    got = lax.all_to_all(maps, SEQ, split_axis=0, concat_axis=0, tiled=True)
    states = pl.pallas_call(
        prefix_kernel,
        out_shape=jax.ShapeDtypeStruct((n_seq, 16, 128), BF),
        in_specs=[VM],
        out_specs=VM,
        compiler_params=SMALL,
        name="prefix",
    )(got)
    states = lax.all_to_all(states, SEQ, split_axis=0, concat_axis=0, tiled=True)
    full = output_weight.shape[1]
    keep, send = pl.pallas_call(
        functools.partial(norm_kernel, seqs, width),
        out_shape=[jax.ShapeDtypeStruct((width, length), BF), jax.ShapeDtypeStruct((length, full), BF)],
        in_specs=[VM] * 6,
        out_specs=[VM] * 2,
        compiler_params=SMALL,
        name="norm",
    )(states, query, local, norm_gain, norm_bias, output_weight)
    half = swap(send)
    outs = pl.pallas_call(
        functools.partial(sum_kernel, width),
        out_shape=[jax.ShapeDtypeStruct((length, width), F32)] + [jax.ShapeDtypeStruct((length, width), BF)] * 7,
        in_specs=[VM] * 3,
        out_specs=[VM] * 8,
        compiler_params=SMALL,
        name="partial",
    )(keep, half, output_weight)
    parts = {(0, 0): outs[0]}
    for d in (2, 1, 3):
        parts[d, 0] = turn(outs[2 * d], 2 * d)
        parts[d, 1] = swap(outs[2 * d + 1], 2 * d)
    parts[0, 1] = swap(outs[1])
    parts = [parts[d, k] for d in range(4) for k in range(2)]
    out = pl.pallas_call(
        fold_kernel,
        out_shape=jax.ShapeDtypeStruct((seqs, width, length), BF),
        in_specs=[VM] * 8,
        out_specs=VM,
        compiler_params=SMALL,
        name="fold",
    )(*parts)
    return jnp.transpose(out, (0, 2, 1))


def solution(mesh):
    torus = Mesh(mesh.devices.reshape(4, 8, mesh.shape["head"]), ("seq_0", "seq_1", "head"))
    placed = (
        P(None, SEQ, "head"),
        P(),
        P(None, "head"),
        P(None, "head"),
        P(None, "head"),
        P("head"),
        P(),
        P(None, "head"),
        P("head"),
        P(),
        P(None, "head"),
        P("head"),
        P("head"),
        P("head"),
        P("head"),
        P("head", None),
    )
    return jax.shard_map(
        body, mesh=torus, in_specs=placed, out_specs=P(None, SEQ, "head"), check_vma=False
    )
```

```python
import functools
import jax
import jax.numpy as jnp
from jax import lax
from jax.experimental import pallas as pl
from jax.experimental.pallas import tpu as pltpu
from jax.sharding import Mesh
from jax.sharding import PartitionSpec as P

HEAD = 64
SPAN = 64
SEQ = ("seq_0", "seq_1")
BF = jnp.bfloat16
F32 = jnp.float32
EDGE = 16
WORK = 2
VM = pl.BlockSpec(memory_space=pltpu.VMEM)
SMALL = pltpu.CompilerParams(vmem_limit_bytes=20 * 1024 * 1024)


def mm(a, b, ca=1, cb=0):
    return lax.dot_general(a, b, (((ca,), (cb,)), ((), ())), preferred_element_type=F32)


def split3(a):
    hi = a.astype(BF)
    rest = a - hi.astype(F32)
    mid = rest.astype(BF)
    low = (rest - mid.astype(F32)).astype(BF)
    return hi, mid, low


def local_kernel(seqs, length, width, n_head, *refs):
    (p0, p1, p2, p3, p4, p5, p6, p7, mix, wr, wk, wv, wd, wl, up_d, up_l, *vecs) = refs[:20]
    (maps_ref, query_ref, local_ref, xs, vp, vr, vk, vv, vd, vl, vm, sems, mcol,
     la_s, lr_s, rb_s, rk_s, vb_s, be_s, ke_s, ad_s, rd_s, ee_s) = refs[20:]
    pieces = (p0, p1, p2, p3, p4, p5, p6, p7)
    moved = [(wr, vr), (wd, vd), (wk, vk), (wv, vv), (wl, vl), (mix, vm)] + [(p, vp.at[k]) for k, p in enumerate(pieces)]
    copies = [pltpu.make_async_copy(a, b, sems.at[i]) for i, (a, b) in enumerate(moved)]
    for c in copies[5:] + copies[:5]:
        c.start()
    cols = seqs * length
    heads = width // HEAD
    me = lax.axis_index("head")
    mate = me + 1 - 2 * lax.rem(me, 2)
    steps = (0, 4, 6, 2)
    copies[5].wait()
    mcol[...] = jnp.transpose(jnp.concatenate([vm[...], jnp.zeros((3, vm.shape[1]), F32)], axis=0))
    block = 64
    lane = lax.broadcasted_iota(jnp.int32, (block, length), 1)
    for k in range(n_head):
        copies[6 + k].wait()
        edge_cols = jnp.transpose(vp[k, seqs * width :, :].astype(F32))
        owner = lax.rem((me if k < 4 else mate) + steps[k % 4], n_head)
        for q in range(width // block):
            start = pl.multiple_of(owner * width + q * block, block)
            m = mcol[pl.ds(start, block), :]
            for s in range(seqs):
                f = s * width + q * block
                cur = vp[k, f : f + block, :].astype(F32)
                r = f // 128
                edge = edge_cols[f % 128 : f % 128 + block, r : r + 1]
                prev = jnp.where(lane == 0, edge, pltpu.roll(cur, 1, 1))
                change = prev - cur
                for j in range(5):
                    xs[j, pl.ds(start, block), s * length : (s + 1) * length] = (
                        cur + change * m[:, j : j + 1]
                    ).astype(BF)
    copies[0].wait()
    recept = mm(vr[...], xs[0])
    copies[1].wait()
    hidden_d = jnp.tanh(mm(vd[...], xs[1])).astype(BF)
    copies[2].wait()
    key_raw = mm(vk[...], xs[2])
    copies[3].wait()
    vb_s[...] = mm(vv[...], xs[3]).astype(BF)
    copies[4].wait()
    hidden_l = mm(vl[...], xs[4]).astype(BF)
    vec_cols = jnp.transpose(jnp.concatenate([v[...].reshape(1, width) for v in vecs] * 2, axis=0))
    vec = lambda i: vec_cols[:, i : i + 1]
    decay = jax.nn.sigmoid(vec(0) + mm(up_d[...], hidden_d, 0, 0)) * (-0.6065306597126334)
    rate = jax.nn.sigmoid(vec(1) + mm(up_l[...], hidden_l, 0, 0))
    scaled = (key_raw * vec(2)).reshape(heads, HEAD, cols)
    unit = (scaled * lax.rsqrt(jnp.sum(scaled * scaled, axis=1, keepdims=True) + 1e-06)).reshape(width, cols)
    key = key_raw * (1.0 + (rate - 1.0) * vec(3))
    si = lax.broadcasted_iota(jnp.int32, (cols, cols), 0)
    ti = lax.broadcasted_iota(jnp.int32, (cols, cols), 1)
    same = si // SPAN == ti // SPAN
    one = lambda c: c.astype(F32)
    upto = one(same & (si <= ti))
    mid = one(same & (si % SPAN < SPAN // 2))
    parts = split3(decay)

    def summed(w):
        w = w.astype(BF)
        return mm(parts[0], w) + mm(parts[1], w) + mm(parts[2], w)

    rel = summed(upto - mid)
    e_mid = jnp.exp(summed(mid))
    e_tail = jnp.exp(summed(one(same) - mid))
    shrink = jnp.exp(-rel)
    l_alpha = -unit * jnp.exp(rel - decay)
    l_recept = recept * jnp.exp(rel)
    r_beta = unit * rate * shrink
    r_key = key * shrink
    be_s[...] = (e_tail * r_beta).astype(BF)
    ke_s[...] = (e_tail * r_key).astype(BF)
    ad_s[...] = e_mid * l_alpha
    rd_s[...] = e_mid * l_recept
    ee_s[...] = e_mid * e_tail
    la_s[...] = l_alpha.astype(BF)
    lr_s[...] = l_recept.astype(BF)
    rb_s[...] = r_beta.astype(BF)
    rk_s[...] = r_key.astype(BF)

    gs = lax.broadcasted_iota(jnp.int32, (2 * length, 2 * length), 0) % length
    gt0 = lax.broadcasted_iota(jnp.int32, (2 * length, 2 * length), 1)
    gt = gt0 % length
    keep = (gs // SPAN == gt // SPAN) & ((gs < gt) | ((gt0 >= length) & (gs == gt)))
    first_lane = lax.broadcasted_iota(jnp.int32, (HEAD, length), 1) < SPAN
    ei = lax.broadcasted_iota(jnp.int32, (HEAD, 2 * HEAD), 0)
    ej = lax.broadcasted_iota(jnp.int32, (HEAD, 2 * HEAD), 1)
    eye = ei == ej
    half = HEAD // WORK
    levels = SPAN.bit_length() - 1

    pairs = [(s, h) for s in range(seqs) for h in range(heads)]

    def cut(a, u):
        s, h = u
        return a[h * HEAD : (h + 1) * HEAD, s * length : (s + 1) * length]

    side = lambda a, b: jnp.concatenate([a, b], axis=1)
    pile = lambda a, b: jnp.concatenate([a, b], axis=0)
    pair_sums = [mm(side(cut(rb_s, u), cut(rk_s, u)), side(cut(la_s, u), cut(lr_s, u)), 0, 0) for u in pairs]
    pair_sums = [jnp.where(keep, g, 0.0).astype(BF) for g in pair_sums]
    powers = [g[:length, :length] for g in pair_sums]
    values = [cut(vb_s, u) for u in pairs]
    sols = [mm(v, g[length:, :length]) for v, g in zip(values, pair_sums)]
    sols = [pile(cut(ad_s, u), x) for u, x in zip(pairs, sols)]
    count = range(len(pairs))
    for level in range(levels - 1):
        steps_y = [mm(pile(sols[i].astype(BF), powers[i]), powers[i]) for i in count]
        sols = [sols[i] + steps_y[i][: 2 * HEAD] for i in count]
        powers = [steps_y[i][2 * HEAD :].astype(BF) for i in count]
    steps_y = [mm(sols[i].astype(BF), powers[i]) for i in count]
    sols = [(sols[i] + steps_y[i]).astype(BF) for i in count]
    rhs = [side(x, pile(jnp.zeros_like(v), v)) for x, v in zip(sols, values)]
    ends = []
    for u in pairs:
        be, ke = cut(be_s, u), cut(ke_s, u)
        zero = jnp.zeros_like(be)
        ends.append(
            pile(
                side(jnp.where(first_lane, be, zero), jnp.where(first_lane, ke, zero)),
                side(jnp.where(first_lane, zero, be), jnp.where(first_lane, zero, ke)),
            )
        )
    both = [mm(e, r, 1, 1) for e, r in zip(ends, rhs)]
    seen = [mm(r, g[:, length:]) for r, g in zip(rhs, pair_sums)]
    lasts = [cut(ee_s, u) for u in pairs]
    m0 = [(y[:HEAD] + jnp.where(eye, last[:, 0:1], 0.0)).astype(BF) for y, last in zip(both, lasts)]
    m1 = [y[HEAD:] + jnp.where(eye, last[:, SPAN : SPAN + 1], 0.0) for y, last in zip(both, lasts)]
    query = [cut(rd_s, u) + y[:HEAD] for u, y in zip(pairs, seen)]
    join = [mm(m1[i][:, :HEAD].astype(BF), m0[i]) for i in count]
    late = [mm(m0[i], query[i].astype(BF), 0, 0) for i in count]
    for p in count:
        total = join[p] + jnp.where(ej >= HEAD, m1[p], 0.0) - jnp.where(eye, 1.0, 0.0)
        packed = side(total[:32, :HEAD], total[32:, :HEAD]).astype(BF)
        for w in range(WORK):
            part = total[:, HEAD + w * half : HEAD + (w + 1) * half]
            block = jnp.concatenate([part[16 * i : 16 * i + 16] for i in range(4)], axis=1).astype(BF)
            maps_ref[p * WORK + w, 0:32, :] = packed
            maps_ref[p * WORK + w, 32:48, :] = block
    for p in count:
        query_ref[p] = jnp.where(first_lane, query[p], late[p][:HEAD]).astype(BF)
        local_ref[p] = jnp.where(first_lane, seen[p][HEAD:], seen[p][HEAD:] + late[p][HEAD:])
    for w in range(seqs * heads * WORK, maps_ref.shape[0]):
        maps_ref[w] = jnp.zeros(maps_ref.shape[1:], BF)


def edge_kernel(x_ref, out_ref):
    length = x_ref.shape[1]
    rows = []
    for r in range(x_ref.shape[0] // 128):
        block = jnp.transpose(x_ref[r * 128 : (r + 1) * 128, :].astype(F32))
        rows.append(block[length - 1 :, :])
    rows.append(jnp.zeros((EDGE - len(rows), 128), F32))
    out_ref[...] = jnp.concatenate(rows, axis=0).astype(BF)


def pack_kernel(x_ref, edge_ref, out_ref):
    rows = x_ref.shape[0]
    out_ref[0:rows, :] = x_ref[...]
    out_ref[rows:, :] = edge_ref[...]


def call_local(dims, near, far, mix, wr, wk, wv, wd, wl, up_d, up_l, vecs, n_seq):
    seqs, width, length = dims
    n_head = len(near) + len(far)
    wide = n_head * width
    low = wd.shape[0]
    cols = seqs * length
    pairs = seqs * (width // HEAD)
    any_ = pl.BlockSpec(memory_space=pltpu.HBM)
    return pl.pallas_call(
        functools.partial(local_kernel, seqs, length, width, n_head),
        out_shape=[
            jax.ShapeDtypeStruct((n_seq, 48, 128), BF),
            jax.ShapeDtypeStruct((pairs, HEAD, length), BF),
            jax.ShapeDtypeStruct((pairs, HEAD, length), F32),
        ],
        in_specs=[any_] * 14 + [VM] * 6,
        out_specs=[VM] * 3,
        scratch_shapes=[
            pltpu.VMEM((5, wide, cols), BF),
            pltpu.VMEM((n_head, seqs * width + EDGE, length), BF),
            *[pltpu.VMEM((width, wide), BF)] * 3,
            *[pltpu.VMEM((low, wide), BF)] * 2,
            pltpu.VMEM(mix.shape, F32),
            pltpu.SemaphoreType.DMA((14,)),
            pltpu.VMEM((wide, 8), F32),
            *[pltpu.VMEM((width, cols), BF)] * 7,
            *[pltpu.VMEM((width, cols), F32)] * 3,
        ],
        name="local",
    )(*near, *far, mix, wr, wk, wv, wd, wl, up_d, up_l, *vecs)


def prefix_kernel(maps_ref, states_ref):
    steps = maps_ref.shape[0]
    group = 8
    groups = steps // group
    half = HEAD // WORK
    eye = (
        lax.broadcasted_iota(jnp.int32, (HEAD, HEAD), 0) == lax.broadcasted_iota(jnp.int32, (HEAD, HEAD), 1)
    ).astype(F32)
    start = jnp.concatenate([eye, jnp.zeros((HEAD, half), F32)], axis=1)

    def load(i):
        packed = maps_ref[i, 0:32, :]
        trans = jnp.concatenate([packed[:, :HEAD], packed[:, HEAD:]], axis=0)
        block = maps_ref[i, 32:48, :]
        incr = jnp.concatenate([block[:, 32 * j : 32 * j + 32] for j in range(4)], axis=0).astype(F32)
        return trans, incr

    run = [start] * groups
    seen = {}
    for i in range(group):
        for g in range(groups):
            seen[g, i] = run[g]
            trans, incr = load(g * group + i)
            add = mm(trans, run[g].astype(BF))
            run[g] = run[g] + add + jnp.concatenate([jnp.zeros((HEAD, HEAD), F32), incr], axis=1)
    state = jnp.zeros((HEAD, half), F32)
    for g in range(groups):
        sb = state.astype(BF)
        for i in range(group):
            a = seen[g, i]
            if i == 0:
                here = state
            else:
                here = state + mm((a[:, :HEAD] - eye).astype(BF), sb) + a[:, HEAD:]
            states_ref[g * group + i] = jnp.concatenate([here[16 * j : 16 * j + 16] for j in range(4)], axis=1).astype(BF)
        state = state + mm((run[g][:, :HEAD] - eye).astype(BF), sb) + run[g][:, HEAD:]


def norm_kernel(seqs, width, states_ref, query_ref, local_ref, gain, bias, w_out, keep_ref, send_ref):
    heads = width // HEAD
    core = lax.rem(lax.axis_index("head"), 2)
    vec_cols = jnp.transpose(jnp.concatenate([v[...].reshape(1, width) for v in (gain, bias)] * 4, axis=0))
    for s in range(seqs):
        blocks = []
        for h in range(heads):
            p = s * heads + h
            halves = []
            for w in range(WORK):
                block = states_ref[p * WORK + w]
                halves.append(jnp.concatenate([block[:, 32 * j : 32 * j + 32] for j in range(4)], axis=0))
            state = jnp.concatenate(halves, axis=1)
            out = mm(state, query_ref[p], 0, 0) + local_ref[p]
            centred = out - jnp.mean(out, axis=0, keepdims=True)
            spread = jnp.mean(centred * centred, axis=0, keepdims=True)
            blocks.append(centred * lax.rsqrt(spread + 0.00064))
        normed = (jnp.concatenate(blocks, axis=0) * vec_cols[:, 0:1] + vec_cols[:, 1:2]).astype(BF)

        @pl.when(core == s)
        def _():
            keep_ref[...] = normed

        @pl.when(core != s)
        def _():
            send_ref[...] = mm(normed, w_out[...], 0, 0).astype(BF)


def sum_kernel(width, keep_ref, got_ref, w_out, *outs):
    wide = 2 * width
    me = lax.axis_index("head")
    x, c = me // 2, lax.rem(me, 2)
    for i in range(4):
        block = lax.rem(x + i, 4)
        cols = pl.ds(pl.multiple_of(block * wide, 128), wide)
        total = mm(keep_ref[...], w_out[:, cols], 0, 0) + got_ref[:, cols].astype(F32)
        total = jnp.transpose(total)
        low, high = total[:width], total[width:]
        same, cross = outs[2 * i], outs[2 * i + 1]
        same[...] = jnp.where(c == 0, low, high).astype(same.dtype)
        cross[...] = jnp.where(c == 0, high, low).astype(cross.dtype)


def fold_kernel(*refs):
    out_ref = refs[-1]
    c = lax.rem(lax.axis_index("head"), 2)
    for i, slot in ((0, c), (1, 1 - c)):
        total = refs[i][...].astype(F32)
        for k in (1, 2, 3):
            total = total + refs[2 * k + i][...].astype(F32)
        out_ref[slot] = total.astype(BF)


def body(
    tokens,
    token_mix,
    receptance,
    key_weight,
    value_weight,
    decay_base,
    decay_down_matrix,
    decay_up_matrix,
    learn_base,
    learning_down_matrix,
    learning_up_matrix,
    key_scale,
    key_blend,
    norm_gain,
    norm_bias,
    output_weight,
):
    seqs, length, width = tokens.shape
    n_head = lax.axis_size("head")
    n_seq = lax.axis_size("seq_0") * lax.axis_size("seq_1")

    def turn(v, d):
        return lax.ppermute(v, "head", [(i, (i + d) % n_head) for i in range(n_head)])

    def swap(v, d=0):
        return lax.ppermute(v, "head", [(i, ((i + d) % n_head) ^ 1) for i in range(n_head)])

    turned = jnp.transpose(tokens, (0, 2, 1)).reshape(seqs * width, length)
    edge = pl.pallas_call(
        edge_kernel,
        out_shape=jax.ShapeDtypeStruct((EDGE, length), BF),
        in_specs=[VM],
        out_specs=VM,
        compiler_params=SMALL,
        name="edge",
    )(turned)
    edge = lax.ppermute(edge, SEQ, [(i, i + 1) for i in range(n_seq - 1)])
    packed = pl.pallas_call(
        pack_kernel,
        out_shape=jax.ShapeDtypeStruct((seqs * width + EDGE, length), BF),
        in_specs=[VM] * 2,
        out_specs=VM,
        compiler_params=SMALL,
        name="pack",
    )(turned, edge)
    near = [packed] + [turn(packed, d) for d in (4, 2, 6)]
    far = [swap(a) for a in near]
    maps, query, local = call_local(
        (seqs, width, length), near, far, token_mix, receptance.T, key_weight.T, value_weight.T,
        decay_down_matrix.T, learning_down_matrix.T, decay_up_matrix, learning_up_matrix,
        (decay_base, learn_base, key_scale, key_blend), n_seq,
    )
    got = lax.all_to_all(maps, SEQ, split_axis=0, concat_axis=0, tiled=True)
    states = pl.pallas_call(
        prefix_kernel,
        out_shape=jax.ShapeDtypeStruct((n_seq, 16, 128), BF),
        in_specs=[VM],
        out_specs=VM,
        compiler_params=SMALL,
        name="prefix",
    )(got)
    states = lax.all_to_all(states, SEQ, split_axis=0, concat_axis=0, tiled=True)
    full = output_weight.shape[1]
    keep, send = pl.pallas_call(
        functools.partial(norm_kernel, seqs, width),
        out_shape=[jax.ShapeDtypeStruct((width, length), BF), jax.ShapeDtypeStruct((length, full), BF)],
        in_specs=[VM] * 6,
        out_specs=[VM] * 2,
        compiler_params=SMALL,
        name="norm",
    )(states, query, local, norm_gain, norm_bias, output_weight)
    half = swap(send)
    outs = pl.pallas_call(
        functools.partial(sum_kernel, width),
        out_shape=[jax.ShapeDtypeStruct((width, length), F32)] + [jax.ShapeDtypeStruct((width, length), BF)] * 7,
        in_specs=[VM] * 3,
        out_specs=[VM] * 8,
        compiler_params=SMALL,
        name="partial",
    )(keep, half, output_weight)
    parts = {(0, 0): outs[0]}
    for d in (2, 1, 3):
        parts[d, 0] = turn(outs[2 * d], 2 * d)
        parts[d, 1] = swap(outs[2 * d + 1], 2 * d)
    parts[0, 1] = swap(outs[1])
    parts = [parts[d, k] for d in range(4) for k in range(2)]
    out = pl.pallas_call(
        fold_kernel,
        out_shape=jax.ShapeDtypeStruct((seqs, width, length), BF),
        in_specs=[VM] * 8,
        out_specs=VM,
        compiler_params=SMALL,
        name="fold",
    )(*parts)
    return jnp.transpose(out, (0, 2, 1))


def solution(mesh):
    torus = Mesh(mesh.devices.reshape(4, 8, mesh.shape["head"]), ("seq_0", "seq_1", "head"))
    placed = (
        P(None, SEQ, "head"),
        P(),
        P(None, "head"),
        P(None, "head"),
        P(None, "head"),
        P("head"),
        P(),
        P(None, "head"),
        P("head"),
        P(),
        P(None, "head"),
        P("head"),
        P("head"),
        P("head"),
        P("head"),
        P("head", None),
    )
    return jax.shard_map(
        body, mesh=torus, in_specs=placed, out_specs=P(None, SEQ, "head"), check_vma=False
    )
```

```python
import functools
import jax
import jax.numpy as jnp
from jax import lax
from jax.experimental import pallas as pl
from jax.experimental.pallas import tpu as pltpu
from jax.sharding import Mesh
from jax.sharding import PartitionSpec as P

HEAD = 64
SPAN = 64
SEQ = ("seq_0", "seq_1")
BF = jnp.bfloat16
F32 = jnp.float32
EDGE = 16
EST = 10**9
LOCAL_LIMIT = 24 * 1024 * 1024
WORK = 2
VM = pl.BlockSpec(memory_space=pltpu.VMEM)
SMALL = pltpu.CompilerParams(vmem_limit_bytes=20 * 1024 * 1024)


def mm(a, b, ca=1, cb=0):
    return lax.dot_general(a, b, (((ca,), (cb,)), ((), ())), preferred_element_type=F32)


def split3(a):
    hi = a.astype(BF)
    rest = a - hi.astype(F32)
    mid = rest.astype(BF)
    low = (rest - mid.astype(F32)).astype(BF)
    return hi, mid, low


def local_kernel(seqs, length, width, n_head, *refs):
    (p0, p1, p2, p3, p4, p5, p6, p7, mix, wr, wk, wv, wd, wl, up_d, up_l, *vecs) = refs[:20]
    (maps_ref, query_ref, local_ref, xs, mcol, rc_s, kr_s, hd_s, hl_s,
     la_s, lr_s, rb_s, rk_s, vb_s, be_s, ke_s, ad_s, rd_s, ee_s) = refs[20:]
    pieces = (p0, p1, p2, p3, p4, p5, p6, p7)
    cols = seqs * length
    heads = width // HEAD
    me = lax.axis_index("head")
    mate = me + 1 - 2 * lax.rem(me, 2)
    steps = (0, 4, 6, 2)
    mcol[...] = jnp.transpose(jnp.concatenate([mix[...], jnp.zeros((3, mix.shape[1]), F32)], axis=0))
    block = 64
    lane = lax.broadcasted_iota(jnp.int32, (block, length), 1)
    for k in range(n_head):

        @pl.when(me >= 0)
        def _(k=k):
            edge_cols = jnp.transpose(pieces[k][seqs * width :, :].astype(F32))
            owner = lax.rem((me if k < 4 else mate) + steps[k % 4], n_head)
            for q in range(width // block):
                start = pl.multiple_of(owner * width + q * block, block)
                m = mcol[pl.ds(start, block), :]
                for s in range(seqs):
                    f = s * width + q * block
                    cur = pieces[k][f : f + block, :].astype(F32)
                    r = f // 128
                    edge = edge_cols[f % 128 : f % 128 + block, r : r + 1]
                    prev = jnp.where(lane == 0, edge, pltpu.roll(cur, 1, 1))
                    change = prev - cur
                    for j in range(5):
                        xs[j, pl.ds(start, block), s * length : (s + 1) * length] = (
                            cur + change * m[:, j : j + 1]
                        ).astype(BF)

    @pl.when(me >= 0)
    def _():
        rc_s[...] = mm(wr[...], xs[0])

    @pl.when(me >= 0)
    def _():
        hd_s[...] = jnp.tanh(mm(wd[...], xs[1])).astype(BF)

    @pl.when(me >= 0)
    def _():
        kr_s[...] = mm(wk[...], xs[2])

    @pl.when(me >= 0)
    def _():
        vb_s[...] = mm(wv[...], xs[3]).astype(BF)

    @pl.when(me >= 0)
    def _():
        hl_s[...] = mm(wl[...], xs[4]).astype(BF)

    @pl.when(me >= 0)
    def _():
        recept, key_raw, hidden_d, hidden_l = rc_s[...], kr_s[...], hd_s[...], hl_s[...]
        vec_cols = jnp.transpose(jnp.concatenate([v[...].reshape(1, width) for v in vecs] * 2, axis=0))
        vec = lambda i: vec_cols[:, i : i + 1]
        decay = jax.nn.sigmoid(vec(0) + mm(up_d[...], hidden_d, 0, 0)) * (-0.6065306597126334)
        rate = jax.nn.sigmoid(vec(1) + mm(up_l[...], hidden_l, 0, 0))
        scaled = (key_raw * vec(2)).reshape(heads, HEAD, cols)
        unit = (scaled * lax.rsqrt(jnp.sum(scaled * scaled, axis=1, keepdims=True) + 1e-06)).reshape(width, cols)
        key = key_raw * (1.0 + (rate - 1.0) * vec(3))
        si = lax.broadcasted_iota(jnp.int32, (cols, cols), 0)
        ti = lax.broadcasted_iota(jnp.int32, (cols, cols), 1)
        same = si // SPAN == ti // SPAN
        one = lambda c: c.astype(F32)
        upto = one(same & (si <= ti))
        mid = one(same & (si % SPAN < SPAN // 2))
        parts = split3(decay)

        def summed(w):
            w = w.astype(BF)
            return mm(parts[0], w) + mm(parts[1], w) + mm(parts[2], w)

        rel = summed(upto - mid)
        e_mid = jnp.exp(summed(mid))
        e_tail = jnp.exp(summed(one(same) - mid))
        shrink = jnp.exp(-rel)
        l_alpha = -unit * jnp.exp(rel - decay)
        l_recept = recept * jnp.exp(rel)
        r_beta = unit * rate * shrink
        r_key = key * shrink
        be_s[...] = (e_tail * r_beta).astype(BF)
        ke_s[...] = (e_tail * r_key).astype(BF)
        ad_s[...] = e_mid * l_alpha
        rd_s[...] = e_mid * l_recept
        ee_s[...] = e_mid * e_tail
        la_s[...] = l_alpha.astype(BF)
        lr_s[...] = l_recept.astype(BF)
        rb_s[...] = r_beta.astype(BF)
        rk_s[...] = r_key.astype(BF)

    @pl.when(me >= 0)
    def _():
        gs = lax.broadcasted_iota(jnp.int32, (2 * length, 2 * length), 0) % length
        gt0 = lax.broadcasted_iota(jnp.int32, (2 * length, 2 * length), 1)
        gt = gt0 % length
        keep = (gs // SPAN == gt // SPAN) & ((gs < gt) | ((gt0 >= length) & (gs == gt)))
        first_lane = lax.broadcasted_iota(jnp.int32, (HEAD, length), 1) < SPAN
        ei = lax.broadcasted_iota(jnp.int32, (HEAD, 2 * HEAD), 0)
        ej = lax.broadcasted_iota(jnp.int32, (HEAD, 2 * HEAD), 1)
        eye = ei == ej
        half = HEAD // WORK
        levels = SPAN.bit_length() - 1

        pairs = [(s, h) for s in range(seqs) for h in range(heads)]

        def cut(a, u):
            s, h = u
            return a[h * HEAD : (h + 1) * HEAD, s * length : (s + 1) * length]

        side = lambda a, b: jnp.concatenate([a, b], axis=1)
        pile = lambda a, b: jnp.concatenate([a, b], axis=0)
        pair_sums = [mm(side(cut(rb_s, u), cut(rk_s, u)), side(cut(la_s, u), cut(lr_s, u)), 0, 0) for u in pairs]
        pair_sums = [jnp.where(keep, g, 0.0).astype(BF) for g in pair_sums]
        powers = [g[:length, :length] for g in pair_sums]
        values = [cut(vb_s, u) for u in pairs]
        sols = [mm(v, g[length:, :length]) for v, g in zip(values, pair_sums)]
        sols = [pile(cut(ad_s, u), x) for u, x in zip(pairs, sols)]
        count = range(len(pairs))
        for level in range(levels - 1):
            steps_y = [mm(pile(sols[i].astype(BF), powers[i]), powers[i]) for i in count]
            sols = [sols[i] + steps_y[i][: 2 * HEAD] for i in count]
            powers = [steps_y[i][2 * HEAD :].astype(BF) for i in count]
        steps_y = [mm(sols[i].astype(BF), powers[i]) for i in count]
        sols = [(sols[i] + steps_y[i]).astype(BF) for i in count]
        rhs = [side(x, pile(jnp.zeros_like(v), v)) for x, v in zip(sols, values)]
        ends = []
        for u in pairs:
            be, ke = cut(be_s, u), cut(ke_s, u)
            zero = jnp.zeros_like(be)
            ends.append(
                pile(
                    side(jnp.where(first_lane, be, zero), jnp.where(first_lane, ke, zero)),
                    side(jnp.where(first_lane, zero, be), jnp.where(first_lane, zero, ke)),
                )
            )
        both = [mm(e, r, 1, 1) for e, r in zip(ends, rhs)]
        seen = [mm(r, g[:, length:]) for r, g in zip(rhs, pair_sums)]
        lasts = [cut(ee_s, u) for u in pairs]
        m0 = [(y[:HEAD] + jnp.where(eye, last[:, 0:1], 0.0)).astype(BF) for y, last in zip(both, lasts)]
        m1 = [y[HEAD:] + jnp.where(eye, last[:, SPAN : SPAN + 1], 0.0) for y, last in zip(both, lasts)]
        query = [cut(rd_s, u) + y[:HEAD] for u, y in zip(pairs, seen)]
        join = [mm(m1[i][:, :HEAD].astype(BF), m0[i]) for i in count]
        late = [mm(m0[i], query[i].astype(BF), 0, 0) for i in count]
        for p in count:
            total = join[p] + jnp.where(ej >= HEAD, m1[p], 0.0) - jnp.where(eye, 1.0, 0.0)
            packed = side(total[:32, :HEAD], total[32:, :HEAD]).astype(BF)
            for w in range(WORK):
                part = total[:, HEAD + w * half : HEAD + (w + 1) * half]
                block = jnp.concatenate([part[16 * i : 16 * i + 16] for i in range(4)], axis=1).astype(BF)
                maps_ref[p * WORK + w, 0:32, :] = packed
                maps_ref[p * WORK + w, 32:48, :] = block
        for p in count:
            query_ref[p] = jnp.where(first_lane, query[p], late[p][:HEAD]).astype(BF)
            local_ref[p] = jnp.where(first_lane, seen[p][HEAD:], seen[p][HEAD:] + late[p][HEAD:])

    for w in range(seqs * heads * WORK, maps_ref.shape[0]):
        maps_ref[w] = jnp.zeros(maps_ref.shape[1:], BF)


def edge_kernel(x_ref, out_ref):
    length = x_ref.shape[1]
    rows = []
    for r in range(x_ref.shape[0] // 128):
        block = jnp.transpose(x_ref[r * 128 : (r + 1) * 128, :].astype(F32))
        rows.append(block[length - 1 :, :])
    rows.append(jnp.zeros((EDGE - len(rows), 128), F32))
    out_ref[...] = jnp.concatenate(rows, axis=0).astype(BF)


def pack_kernel(x_ref, edge_ref, out_ref):
    rows = x_ref.shape[0]
    out_ref[0:rows, :] = x_ref[...]
    out_ref[rows:, :] = edge_ref[...]


def call_local(dims, near, far, mix, wr, wk, wv, wd, wl, up_d, up_l, vecs, n_seq):
    seqs, width, length = dims
    n_head = len(near) + len(far)
    wide = n_head * width
    cols = seqs * length
    pairs = seqs * (width // HEAD)
    return pl.pallas_call(
        functools.partial(local_kernel, seqs, length, width, n_head),
        out_shape=[
            jax.ShapeDtypeStruct((n_seq, 48, 128), BF),
            jax.ShapeDtypeStruct((pairs, HEAD, length), BF),
            jax.ShapeDtypeStruct((pairs, HEAD, length), F32),
        ],
        in_specs=[VM] * 20,
        out_specs=[VM] * 3,
        scratch_shapes=[
            pltpu.VMEM((5, wide, cols), BF),
            pltpu.VMEM((wide, 8), F32),
            *[pltpu.VMEM((width, cols), F32)] * 2,
            *[pltpu.VMEM((wd.shape[0], cols), BF)] * 2,
            *[pltpu.VMEM((width, cols), BF)] * 7,
            *[pltpu.VMEM((width, cols), F32)] * 3,
        ],
        compiler_params=pltpu.CompilerParams(vmem_limit_bytes=LOCAL_LIMIT),
        name="local",
    )(*near, *far, mix, wr, wk, wv, wd, wl, up_d, up_l, *vecs)


def prefix_kernel(maps_ref, states_ref):
    steps = maps_ref.shape[0]
    group = 8
    groups = steps // group
    half = HEAD // WORK
    eye = (
        lax.broadcasted_iota(jnp.int32, (HEAD, HEAD), 0) == lax.broadcasted_iota(jnp.int32, (HEAD, HEAD), 1)
    ).astype(F32)
    start = jnp.concatenate([eye, jnp.zeros((HEAD, half), F32)], axis=1)

    def load(i):
        packed = maps_ref[i, 0:32, :]
        trans = jnp.concatenate([packed[:, :HEAD], packed[:, HEAD:]], axis=0)
        block = maps_ref[i, 32:48, :]
        incr = jnp.concatenate([block[:, 32 * j : 32 * j + 32] for j in range(4)], axis=0).astype(F32)
        return trans, incr

    run = [start] * groups
    seen = {}
    for i in range(group):
        for g in range(groups):
            seen[g, i] = run[g]
            trans, incr = load(g * group + i)
            add = mm(trans, run[g].astype(BF))
            run[g] = run[g] + add + jnp.concatenate([jnp.zeros((HEAD, HEAD), F32), incr], axis=1)
    state = jnp.zeros((HEAD, half), F32)
    for g in range(groups):
        sb = state.astype(BF)
        for i in range(group):
            a = seen[g, i]
            if i == 0:
                here = state
            else:
                here = state + mm((a[:, :HEAD] - eye).astype(BF), sb) + a[:, HEAD:]
            states_ref[g * group + i] = jnp.concatenate([here[16 * j : 16 * j + 16] for j in range(4)], axis=1).astype(BF)
        state = state + mm((run[g][:, :HEAD] - eye).astype(BF), sb) + run[g][:, HEAD:]


def norm_kernel(seqs, width, states_ref, query_ref, local_ref, gain, bias, w_out, keep_ref, send_ref):
    heads = width // HEAD
    core = lax.rem(lax.axis_index("head"), 2)
    vec_cols = jnp.transpose(jnp.concatenate([v[...].reshape(1, width) for v in (gain, bias)] * 4, axis=0))
    for s in range(seqs):
        blocks = []
        for h in range(heads):
            p = s * heads + h
            halves = []
            for w in range(WORK):
                block = states_ref[p * WORK + w]
                halves.append(jnp.concatenate([block[:, 32 * j : 32 * j + 32] for j in range(4)], axis=0))
            state = jnp.concatenate(halves, axis=1)
            out = mm(state, query_ref[p], 0, 0) + local_ref[p]
            centred = out - jnp.mean(out, axis=0, keepdims=True)
            spread = jnp.mean(centred * centred, axis=0, keepdims=True)
            blocks.append(centred * lax.rsqrt(spread + 0.00064))
        normed = (jnp.concatenate(blocks, axis=0) * vec_cols[:, 0:1] + vec_cols[:, 1:2]).astype(BF)

        @pl.when(core == s)
        def _():
            keep_ref[...] = normed

        @pl.when(core != s)
        def _():
            send_ref[...] = mm(normed, w_out[...], 0, 0).astype(BF)


def sum_kernel(width, keep_ref, got_ref, w_out, *outs):
    wide = 2 * width
    me = lax.axis_index("head")
    x, c = me // 2, lax.rem(me, 2)
    for i in range(4):
        block = lax.rem(x + i, 4)
        cols = pl.ds(pl.multiple_of(block * wide, 128), wide)
        total = mm(keep_ref[...], w_out[:, cols], 0, 0) + got_ref[:, cols].astype(F32)
        total = jnp.transpose(total)
        low, high = total[:width], total[width:]
        same, cross = outs[2 * i], outs[2 * i + 1]
        same[...] = jnp.where(c == 0, low, high).astype(same.dtype)
        cross[...] = jnp.where(c == 0, high, low).astype(cross.dtype)


def fold_kernel(*refs):
    out_ref = refs[-1]
    c = lax.rem(lax.axis_index("head"), 2)
    for i, slot in ((0, c), (1, 1 - c)):
        total = refs[i][...].astype(F32)
        for k in (1, 2, 3):
            total = total + refs[2 * k + i][...].astype(F32)
        out_ref[slot] = total.astype(BF)


def body(
    tokens,
    token_mix,
    receptance,
    key_weight,
    value_weight,
    decay_base,
    decay_down_matrix,
    decay_up_matrix,
    learn_base,
    learning_down_matrix,
    learning_up_matrix,
    key_scale,
    key_blend,
    norm_gain,
    norm_bias,
    output_weight,
):
    seqs, length, width = tokens.shape
    n_head = lax.axis_size("head")
    n_seq = lax.axis_size("seq_0") * lax.axis_size("seq_1")

    def turn(v, d):
        return lax.ppermute(v, "head", [(i, (i + d) % n_head) for i in range(n_head)])

    def swap(v, d=0):
        return lax.ppermute(v, "head", [(i, ((i + d) % n_head) ^ 1) for i in range(n_head)])

    turned = jnp.transpose(tokens, (0, 2, 1)).reshape(seqs * width, length)
    edge = pl.pallas_call(
        edge_kernel,
        out_shape=jax.ShapeDtypeStruct((EDGE, length), BF),
        in_specs=[VM],
        out_specs=VM,
        compiler_params=SMALL,
        cost_estimate=pl.CostEstimate(flops=EST, bytes_accessed=EST // 100, transcendentals=0),
        name="edge",
    )(turned)
    edge = lax.ppermute(edge, SEQ, [(i, i + 1) for i in range(n_seq - 1)])
    packed = pl.pallas_call(
        pack_kernel,
        out_shape=jax.ShapeDtypeStruct((seqs * width + EDGE, length), BF),
        in_specs=[VM] * 2,
        out_specs=VM,
        compiler_params=SMALL,
        cost_estimate=pl.CostEstimate(flops=EST, bytes_accessed=EST // 100, transcendentals=0),
        name="pack",
    )(turned, edge)
    near = [packed] + [turn(packed, d) for d in (4, 2, 6)]
    far = [swap(a) for a in near]
    maps, query, local = call_local(
        (seqs, width, length), near, far, token_mix, receptance.T, key_weight.T, value_weight.T,
        decay_down_matrix.T, learning_down_matrix.T, decay_up_matrix, learning_up_matrix,
        (decay_base, learn_base, key_scale, key_blend), n_seq,
    )
    got = lax.all_to_all(maps, SEQ, split_axis=0, concat_axis=0, tiled=True)
    states = pl.pallas_call(
        prefix_kernel,
        out_shape=jax.ShapeDtypeStruct((n_seq, 16, 128), BF),
        in_specs=[VM],
        out_specs=VM,
        compiler_params=SMALL,
        name="prefix",
    )(got)
    states = lax.all_to_all(states, SEQ, split_axis=0, concat_axis=0, tiled=True)
    full = output_weight.shape[1]
    keep, send = pl.pallas_call(
        functools.partial(norm_kernel, seqs, width),
        out_shape=[jax.ShapeDtypeStruct((width, length), BF), jax.ShapeDtypeStruct((length, full), BF)],
        in_specs=[VM] * 6,
        out_specs=[VM] * 2,
        compiler_params=SMALL,
        name="norm",
    )(states, query, local, norm_gain, norm_bias, output_weight)
    half = swap(send)
    outs = pl.pallas_call(
        functools.partial(sum_kernel, width),
        out_shape=[jax.ShapeDtypeStruct((width, length), F32)] + [jax.ShapeDtypeStruct((width, length), BF)] * 7,
        in_specs=[VM] * 3,
        out_specs=[VM] * 8,
        compiler_params=SMALL,
        name="partial",
    )(keep, half, output_weight)
    parts = {(0, 0): outs[0]}
    for d in (2, 1, 3):
        parts[d, 0] = turn(outs[2 * d], 2 * d)
        parts[d, 1] = swap(outs[2 * d + 1], 2 * d)
    parts[0, 1] = swap(outs[1])
    parts = [parts[d, k] for d in range(4) for k in range(2)]
    out = pl.pallas_call(
        fold_kernel,
        out_shape=jax.ShapeDtypeStruct((seqs, width, length), BF),
        in_specs=[VM] * 8,
        out_specs=VM,
        compiler_params=SMALL,
        name="fold",
    )(*parts)
    return jnp.transpose(out, (0, 2, 1))


def solution(mesh):
    torus = Mesh(mesh.devices.reshape(4, 8, mesh.shape["head"]), ("seq_0", "seq_1", "head"))
    placed = (
        P(None, SEQ, "head"),
        P(),
        P(None, "head"),
        P(None, "head"),
        P(None, "head"),
        P("head"),
        P(),
        P(None, "head"),
        P("head"),
        P(),
        P(None, "head"),
        P("head"),
        P("head"),
        P("head"),
        P("head"),
        P("head", None),
    )
    return jax.shard_map(
        body, mesh=torus, in_specs=placed, out_specs=P(None, SEQ, "head"), check_vma=False
    )
```

```python
import functools
import jax
import jax.numpy as jnp
from jax import lax
from jax.experimental import pallas as pl
from jax.experimental.pallas import tpu as pltpu
from jax.sharding import Mesh
from jax.sharding import PartitionSpec as P

HEAD = 64
SPAN = 64
SEQ = ("seq_0", "seq_1")
BF = jnp.bfloat16
F32 = jnp.float32
EDGE = 16
EST = 10**9
LOCAL_LIMIT = 24 * 1024 * 1024
WORK = 2
VM = pl.BlockSpec(memory_space=pltpu.VMEM)
SMALL = pltpu.CompilerParams(vmem_limit_bytes=20 * 1024 * 1024)


def mm(a, b, ca=1, cb=0):
    return lax.dot_general(a, b, (((ca,), (cb,)), ((), ())), preferred_element_type=F32)


def split3(a):
    hi = a.astype(BF)
    rest = a - hi.astype(F32)
    mid = rest.astype(BF)
    low = (rest - mid.astype(F32)).astype(BF)
    return hi, mid, low


def local_kernel(seqs, length, width, n_head, *refs):
    (p0, p1, p2, p3, p4, p5, p6, p7, mix, wr, wk, wv, wd, wl, up_d, up_l, *vecs) = refs[:20]
    (maps_ref, query_ref, local_ref, xs, vp, sems, mcol, rc_s, kr_s, hd_s, hl_s,
     la_s, lr_s, rb_s, rk_s, vb_s, be_s, ke_s, ad_s, rd_s, ee_s) = refs[20:]
    pieces = (p0, p1, p2, p3, p4, p5, p6, p7)
    copies = [pltpu.make_async_copy(p, vp.at[k], sems.at[k]) for k, p in enumerate(pieces)]
    for c in copies:
        c.start()
    cols = seqs * length
    heads = width // HEAD
    me = lax.axis_index("head")
    mate = me + 1 - 2 * lax.rem(me, 2)
    steps = (0, 4, 6, 2)
    mcol[...] = jnp.transpose(jnp.concatenate([mix[...], jnp.zeros((3, mix.shape[1]), F32)], axis=0))
    block = 64
    lane = lax.broadcasted_iota(jnp.int32, (block, length), 1)
    for k in range(n_head):
        copies[k].wait()

        @pl.when(me >= 0)
        def _(k=k):
            edge_cols = jnp.transpose(vp[k, seqs * width :, :].astype(F32))
            owner = lax.rem((me if k < 4 else mate) + steps[k % 4], n_head)
            for q in range(width // block):
                start = pl.multiple_of(owner * width + q * block, block)
                m = mcol[pl.ds(start, block), :]
                for s in range(seqs):
                    f = s * width + q * block
                    cur = vp[k, f : f + block, :].astype(F32)
                    r = f // 128
                    edge = edge_cols[f % 128 : f % 128 + block, r : r + 1]
                    prev = jnp.where(lane == 0, edge, pltpu.roll(cur, 1, 1))
                    change = prev - cur
                    for j in range(5):
                        xs[j, pl.ds(start, block), s * length : (s + 1) * length] = (
                            cur + change * m[:, j : j + 1]
                        ).astype(BF)

    @pl.when(me >= 0)
    def _():
        rc_s[...] = mm(wr[...], xs[0])

    @pl.when(me >= 0)
    def _():
        hd_s[...] = jnp.tanh(mm(wd[...], xs[1])).astype(BF)

    @pl.when(me >= 0)
    def _():
        kr_s[...] = mm(wk[...], xs[2])

    @pl.when(me >= 0)
    def _():
        vb_s[...] = mm(wv[...], xs[3]).astype(BF)

    @pl.when(me >= 0)
    def _():
        hl_s[...] = mm(wl[...], xs[4]).astype(BF)

    @pl.when(me >= 0)
    def _():
        recept, key_raw, hidden_d, hidden_l = rc_s[...], kr_s[...], hd_s[...], hl_s[...]
        vec_cols = jnp.transpose(jnp.concatenate([v[...].reshape(1, width) for v in vecs] * 2, axis=0))
        vec = lambda i: vec_cols[:, i : i + 1]
        decay = jax.nn.sigmoid(vec(0) + mm(up_d[...], hidden_d, 0, 0)) * (-0.6065306597126334)
        rate = jax.nn.sigmoid(vec(1) + mm(up_l[...], hidden_l, 0, 0))
        scaled = (key_raw * vec(2)).reshape(heads, HEAD, cols)
        unit = (scaled * lax.rsqrt(jnp.sum(scaled * scaled, axis=1, keepdims=True) + 1e-06)).reshape(width, cols)
        key = key_raw * (1.0 + (rate - 1.0) * vec(3))
        si = lax.broadcasted_iota(jnp.int32, (cols, cols), 0)
        ti = lax.broadcasted_iota(jnp.int32, (cols, cols), 1)
        same = si // SPAN == ti // SPAN
        one = lambda c: c.astype(F32)
        upto = one(same & (si <= ti))
        mid = one(same & (si % SPAN < SPAN // 2))
        parts = split3(decay)

        def summed(w):
            w = w.astype(BF)
            return mm(parts[0], w) + mm(parts[1], w) + mm(parts[2], w)

        rel = summed(upto - mid)
        e_mid = jnp.exp(summed(mid))
        e_tail = jnp.exp(summed(one(same) - mid))
        shrink = jnp.exp(-rel)
        l_alpha = -unit * jnp.exp(rel - decay)
        l_recept = recept * jnp.exp(rel)
        r_beta = unit * rate * shrink
        r_key = key * shrink
        be_s[...] = (e_tail * r_beta).astype(BF)
        ke_s[...] = (e_tail * r_key).astype(BF)
        ad_s[...] = e_mid * l_alpha
        rd_s[...] = e_mid * l_recept
        ee_s[...] = e_mid * e_tail
        la_s[...] = l_alpha.astype(BF)
        lr_s[...] = l_recept.astype(BF)
        rb_s[...] = r_beta.astype(BF)
        rk_s[...] = r_key.astype(BF)

    @pl.when(me >= 0)
    def _():
        gs = lax.broadcasted_iota(jnp.int32, (2 * length, 2 * length), 0) % length
        gt0 = lax.broadcasted_iota(jnp.int32, (2 * length, 2 * length), 1)
        gt = gt0 % length
        keep = (gs // SPAN == gt // SPAN) & ((gs < gt) | ((gt0 >= length) & (gs == gt)))
        first_lane = lax.broadcasted_iota(jnp.int32, (HEAD, length), 1) < SPAN
        ei = lax.broadcasted_iota(jnp.int32, (HEAD, 2 * HEAD), 0)
        ej = lax.broadcasted_iota(jnp.int32, (HEAD, 2 * HEAD), 1)
        eye = ei == ej
        half = HEAD // WORK
        levels = SPAN.bit_length() - 1

        pairs = [(s, h) for s in range(seqs) for h in range(heads)]

        def cut(a, u):
            s, h = u
            return a[h * HEAD : (h + 1) * HEAD, s * length : (s + 1) * length]

        side = lambda a, b: jnp.concatenate([a, b], axis=1)
        pile = lambda a, b: jnp.concatenate([a, b], axis=0)
        pair_sums = [mm(side(cut(rb_s, u), cut(rk_s, u)), side(cut(la_s, u), cut(lr_s, u)), 0, 0) for u in pairs]
        pair_sums = [jnp.where(keep, g, 0.0).astype(BF) for g in pair_sums]
        powers = [g[:length, :length] for g in pair_sums]
        values = [cut(vb_s, u) for u in pairs]
        sols = [mm(v, g[length:, :length]) for v, g in zip(values, pair_sums)]
        sols = [pile(cut(ad_s, u), x) for u, x in zip(pairs, sols)]
        count = range(len(pairs))
        for level in range(levels - 1):
            steps_y = [mm(pile(sols[i].astype(BF), powers[i]), powers[i]) for i in count]
            sols = [sols[i] + steps_y[i][: 2 * HEAD] for i in count]
            powers = [steps_y[i][2 * HEAD :].astype(BF) for i in count]
        steps_y = [mm(sols[i].astype(BF), powers[i]) for i in count]
        sols = [(sols[i] + steps_y[i]).astype(BF) for i in count]
        rhs = [side(x, pile(jnp.zeros_like(v), v)) for x, v in zip(sols, values)]
        ends = []
        for u in pairs:
            be, ke = cut(be_s, u), cut(ke_s, u)
            zero = jnp.zeros_like(be)
            ends.append(
                pile(
                    side(jnp.where(first_lane, be, zero), jnp.where(first_lane, ke, zero)),
                    side(jnp.where(first_lane, zero, be), jnp.where(first_lane, zero, ke)),
                )
            )
        both = [mm(e, r, 1, 1) for e, r in zip(ends, rhs)]
        seen = [mm(r, g[:, length:]) for r, g in zip(rhs, pair_sums)]
        lasts = [cut(ee_s, u) for u in pairs]
        m0 = [(y[:HEAD] + jnp.where(eye, last[:, 0:1], 0.0)).astype(BF) for y, last in zip(both, lasts)]
        m1 = [y[HEAD:] + jnp.where(eye, last[:, SPAN : SPAN + 1], 0.0) for y, last in zip(both, lasts)]
        query = [cut(rd_s, u) + y[:HEAD] for u, y in zip(pairs, seen)]
        join = [mm(m1[i][:, :HEAD].astype(BF), m0[i]) for i in count]
        late = [mm(m0[i], query[i].astype(BF), 0, 0) for i in count]
        for p in count:
            total = join[p] + jnp.where(ej >= HEAD, m1[p], 0.0) - jnp.where(eye, 1.0, 0.0)
            packed = side(total[:32, :HEAD], total[32:, :HEAD]).astype(BF)
            for w in range(WORK):
                part = total[:, HEAD + w * half : HEAD + (w + 1) * half]
                block = jnp.concatenate([part[16 * i : 16 * i + 16] for i in range(4)], axis=1).astype(BF)
                maps_ref[p * WORK + w, 0:32, :] = packed
                maps_ref[p * WORK + w, 32:48, :] = block
        for p in count:
            query_ref[p] = jnp.where(first_lane, query[p], late[p][:HEAD]).astype(BF)
            local_ref[p] = jnp.where(first_lane, seen[p][HEAD:], seen[p][HEAD:] + late[p][HEAD:])

    for w in range(seqs * heads * WORK, maps_ref.shape[0]):
        maps_ref[w] = jnp.zeros(maps_ref.shape[1:], BF)


def edge_kernel(x_ref, out_ref):
    length = x_ref.shape[1]
    rows = []
    for r in range(x_ref.shape[0] // 128):
        block = jnp.transpose(x_ref[r * 128 : (r + 1) * 128, :].astype(F32))
        rows.append(block[length - 1 :, :])
    rows.append(jnp.zeros((EDGE - len(rows), 128), F32))
    out_ref[...] = jnp.concatenate(rows, axis=0).astype(BF)


def pack_kernel(x_ref, edge_ref, out_ref):
    rows = x_ref.shape[0]
    out_ref[0:rows, :] = x_ref[...]
    out_ref[rows:, :] = edge_ref[...]


def call_local(dims, near, far, mix, wr, wk, wv, wd, wl, up_d, up_l, vecs, n_seq):
    seqs, width, length = dims
    n_head = len(near) + len(far)
    wide = n_head * width
    cols = seqs * length
    pairs = seqs * (width // HEAD)
    return pl.pallas_call(
        functools.partial(local_kernel, seqs, length, width, n_head),
        out_shape=[
            jax.ShapeDtypeStruct((n_seq, 48, 128), BF),
            jax.ShapeDtypeStruct((pairs, HEAD, length), BF),
            jax.ShapeDtypeStruct((pairs, HEAD, length), F32),
        ],
        in_specs=[pl.BlockSpec(memory_space=pl.ANY)] * 8 + [VM] * 12,
        out_specs=[VM] * 3,
        scratch_shapes=[
            pltpu.VMEM((5, wide, cols), BF),
            pltpu.VMEM((n_head, seqs * width + EDGE, length), BF),
            pltpu.SemaphoreType.DMA((n_head,)),
            pltpu.VMEM((wide, 8), F32),
            *[pltpu.VMEM((width, cols), F32)] * 2,
            *[pltpu.VMEM((wd.shape[0], cols), BF)] * 2,
            *[pltpu.VMEM((width, cols), BF)] * 7,
            *[pltpu.VMEM((width, cols), F32)] * 3,
        ],
        compiler_params=pltpu.CompilerParams(vmem_limit_bytes=LOCAL_LIMIT),
        name="local",
    )(*near, *far, mix, wr, wk, wv, wd, wl, up_d, up_l, *vecs)


def prefix_kernel(maps_ref, states_ref):
    steps = maps_ref.shape[0]
    group = 8
    groups = steps // group
    half = HEAD // WORK
    eye = (
        lax.broadcasted_iota(jnp.int32, (HEAD, HEAD), 0) == lax.broadcasted_iota(jnp.int32, (HEAD, HEAD), 1)
    ).astype(F32)
    start = jnp.concatenate([eye, jnp.zeros((HEAD, half), F32)], axis=1)

    def load(i):
        packed = maps_ref[i, 0:32, :]
        trans = jnp.concatenate([packed[:, :HEAD], packed[:, HEAD:]], axis=0)
        block = maps_ref[i, 32:48, :]
        incr = jnp.concatenate([block[:, 32 * j : 32 * j + 32] for j in range(4)], axis=0).astype(F32)
        return trans, incr

    run = [start] * groups
    seen = {}
    for i in range(group):
        for g in range(groups):
            seen[g, i] = run[g]
            trans, incr = load(g * group + i)
            add = mm(trans, run[g].astype(BF))
            run[g] = run[g] + add + jnp.concatenate([jnp.zeros((HEAD, HEAD), F32), incr], axis=1)
    state = jnp.zeros((HEAD, half), F32)
    for g in range(groups):
        sb = state.astype(BF)
        for i in range(group):
            a = seen[g, i]
            if i == 0:
                here = state
            else:
                here = state + mm((a[:, :HEAD] - eye).astype(BF), sb) + a[:, HEAD:]
            states_ref[g * group + i] = jnp.concatenate([here[16 * j : 16 * j + 16] for j in range(4)], axis=1).astype(BF)
        state = state + mm((run[g][:, :HEAD] - eye).astype(BF), sb) + run[g][:, HEAD:]


def norm_kernel(seqs, width, states_ref, query_ref, local_ref, gain, bias, keep_ref, send_ref):
    heads = width // HEAD
    core = lax.rem(lax.axis_index("head"), 2)
    vec_cols = jnp.transpose(jnp.concatenate([v[...].reshape(1, width) for v in (gain, bias)] * 4, axis=0))
    for s in range(seqs):
        blocks = []
        for h in range(heads):
            p = s * heads + h
            halves = []
            for w in range(WORK):
                block = states_ref[p * WORK + w]
                halves.append(jnp.concatenate([block[:, 32 * j : 32 * j + 32] for j in range(4)], axis=0))
            state = jnp.concatenate(halves, axis=1)
            out = mm(state, query_ref[p], 0, 0) + local_ref[p]
            centred = out - jnp.mean(out, axis=0, keepdims=True)
            spread = jnp.mean(centred * centred, axis=0, keepdims=True)
            blocks.append(centred * lax.rsqrt(spread + 0.00064))
        normed = (jnp.concatenate(blocks, axis=0) * vec_cols[:, 0:1] + vec_cols[:, 1:2]).astype(BF)

        @pl.when(core == s)
        def _():
            keep_ref[...] = normed

        @pl.when(core != s)
        def _():
            send_ref[...] = normed


def sum_kernel(width, keep_ref, got_ref, w_out, w_far, *outs):
    wide = 2 * width
    me = lax.axis_index("head")
    x, c = me // 2, lax.rem(me, 2)
    for i in range(4):
        block = lax.rem(x + i, 4)
        cols = pl.ds(pl.multiple_of(block * wide, 128), wide)
        total = mm(keep_ref[...], w_out[:, cols], 0, 0) + mm(got_ref[...], w_far[:, cols], 0, 0)
        total = jnp.transpose(total)
        low, high = total[:width], total[width:]
        same, cross = outs[2 * i], outs[2 * i + 1]
        same[...] = jnp.where(c == 0, low, high).astype(same.dtype)
        cross[...] = jnp.where(c == 0, high, low).astype(cross.dtype)


def fold_kernel(*refs):
    out_ref = refs[-1]
    c = lax.rem(lax.axis_index("head"), 2)
    for i, slot in ((0, c), (1, 1 - c)):
        total = refs[i][...].astype(F32)
        for k in (1, 2, 3):
            total = total + refs[2 * k + i][...].astype(F32)
        out_ref[slot] = total.astype(BF)


def body(
    tokens,
    token_mix,
    receptance,
    key_weight,
    value_weight,
    decay_base,
    decay_down_matrix,
    decay_up_matrix,
    learn_base,
    learning_down_matrix,
    learning_up_matrix,
    key_scale,
    key_blend,
    norm_gain,
    norm_bias,
    output_weight,
):
    seqs, length, width = tokens.shape
    n_head = lax.axis_size("head")
    n_seq = lax.axis_size("seq_0") * lax.axis_size("seq_1")

    def turn(v, d):
        return lax.ppermute(v, "head", [(i, (i + d) % n_head) for i in range(n_head)])

    def swap(v, d=0):
        return lax.ppermute(v, "head", [(i, ((i + d) % n_head) ^ 1) for i in range(n_head)])

    turned = jnp.transpose(tokens, (0, 2, 1)).reshape(seqs * width, length)
    edge = pl.pallas_call(
        edge_kernel,
        out_shape=jax.ShapeDtypeStruct((EDGE, length), BF),
        in_specs=[VM],
        out_specs=VM,
        compiler_params=SMALL,
        cost_estimate=pl.CostEstimate(flops=EST, bytes_accessed=EST // 100, transcendentals=0),
        name="edge",
    )(turned)
    edge = lax.ppermute(edge, SEQ, [(i, i + 1) for i in range(n_seq - 1)])
    packed = pl.pallas_call(
        pack_kernel,
        out_shape=jax.ShapeDtypeStruct((seqs * width + EDGE, length), BF),
        in_specs=[VM] * 2,
        out_specs=VM,
        compiler_params=SMALL,
        cost_estimate=pl.CostEstimate(flops=EST, bytes_accessed=EST // 100, transcendentals=0),
        name="pack",
    )(turned, edge)
    weight_far = swap(output_weight)
    near = [packed] + [turn(packed, d) for d in (4, 2, 6)]
    far = [swap(a) for a in near]
    maps, query, local = call_local(
        (seqs, width, length), near, far, token_mix, receptance.T, key_weight.T, value_weight.T,
        decay_down_matrix.T, learning_down_matrix.T, decay_up_matrix, learning_up_matrix,
        (decay_base, learn_base, key_scale, key_blend), n_seq,
    )
    got = lax.all_to_all(maps, SEQ, split_axis=0, concat_axis=0, tiled=True)
    states = pl.pallas_call(
        prefix_kernel,
        out_shape=jax.ShapeDtypeStruct((n_seq, 16, 128), BF),
        in_specs=[VM],
        out_specs=VM,
        compiler_params=SMALL,
        name="prefix",
    )(got)
    states = lax.all_to_all(states, SEQ, split_axis=0, concat_axis=0, tiled=True)
    keep, send = pl.pallas_call(
        functools.partial(norm_kernel, seqs, width),
        out_shape=[jax.ShapeDtypeStruct((width, length), BF)] * 2,
        in_specs=[VM] * 5,
        out_specs=[VM] * 2,
        compiler_params=SMALL,
        name="norm",
    )(states, query, local, norm_gain, norm_bias)
    half = swap(send)
    outs = pl.pallas_call(
        functools.partial(sum_kernel, width),
        out_shape=[jax.ShapeDtypeStruct((width, length), F32)] + [jax.ShapeDtypeStruct((width, length), BF)] * 7,
        in_specs=[VM] * 4,
        out_specs=[VM] * 8,
        compiler_params=SMALL,
        name="partial",
    )(keep, half, output_weight, weight_far)
    parts = {(0, 0): outs[0]}
    for d in (2, 1, 3):
        parts[d, 0] = turn(outs[2 * d], 2 * d)
        parts[d, 1] = swap(outs[2 * d + 1], 2 * d)
    parts[0, 1] = swap(outs[1])
    parts = [parts[d, k] for d in range(4) for k in range(2)]
    out = pl.pallas_call(
        fold_kernel,
        out_shape=jax.ShapeDtypeStruct((seqs, width, length), BF),
        in_specs=[VM] * 8,
        out_specs=VM,
        compiler_params=SMALL,
        name="fold",
    )(*parts)
    return jnp.transpose(out, (0, 2, 1))


def solution(mesh):
    torus = Mesh(mesh.devices.reshape(4, 8, mesh.shape["head"]), ("seq_0", "seq_1", "head"))
    placed = (
        P(None, SEQ, "head"),
        P(),
        P(None, "head"),
        P(None, "head"),
        P(None, "head"),
        P("head"),
        P(),
        P(None, "head"),
        P("head"),
        P(),
        P(None, "head"),
        P("head"),
        P("head"),
        P("head"),
        P("head"),
        P("head", None),
    )
    return jax.shard_map(
        body, mesh=torus, in_specs=placed, out_specs=P(None, SEQ, "head"), check_vma=False
    )
```
